128 devices in a mesh: expert: 16 (over y_lo, x, core), row: 2 (over y_hi), col: 4 (over z).
Axes of the slice: x: 4, y: 4 (y_hi: 2, y_lo: 2; y = y_hi * 2 + y_lo), z: 4, core: 2. Of those that a mesh axis runs over, the one named last changes fastest.
Arguments:
- weights: bfloat16 [16, 4096, 7168], P('expert', 'row', 'col'), may hold values from -210 to 210
- inputs: bfloat16 [16, 1024, 4096], P('expert', ('row', 'col')), may hold values from -80 to 80
- cotangents: bfloat16 [16, 1024, 7168], P('expert', ('row', 'col')), may hold values from -150 to 150
- row_state: float32 [16, 4096], P('expert', 'row'), may hold values from 0.00089 to 0.91
- col_state: float32 [16, 7168], P('expert', 'col'), may hold values from 0.00089 to 0.91
Outputs:
- scaled_update: float32 [16, 4096, 7168], P('expert', 'row', 'col')
- new_row_state: float32 [16, 4096], P('expert', 'row')
- new_col_state: float32 [16, 7168], P('expert', 'col')
The draws below stay inside these ranges and needn't reach their ends.
All inputs are finite; a program needn't handle non-finite values.
Results may differ from the reference program's by a relative error of at most 0.0003.
Values may be sent and summed in bfloat16 or wider, within the bound.
A program may use at most 128 MiB of HBM per device.

```python
import math
import jax
import jax.numpy as jnp
from jax import lax

D = 4096
FF = 7168
STEP = 10
MATS = 16
TOK = 1024


def spread(key, array_shape, low_end, high_end):
    return jnp.exp(jax.random.uniform(key, array_shape, jnp.float32, math.log(low_end), math.log(high_end)))


def rising(length, factor):
    return factor ** (jnp.arange(length, dtype=jnp.float32) / length)


def draw_inputs(key, part):
    feature = spread(jax.random.fold_in(key, 11), (MATS, 1, D), 1.0, 10.0)
    values = jax.random.truncated_normal(jax.random.fold_in(key, 14), -6.0, 6.0, (MATS, TOK, D)) * feature * rising(D, 3.0)
    return (0.25 * values).astype(jnp.bfloat16)


def draw_cotangents(key, part):
    column_scale = spread(jax.random.fold_in(key, 21), (MATS, 1, FF), 1.0, 10.0) * rising(FF, 3.0)
    matrix_scale = rising(MATS, 3.0)[:, None, None]
    values = jax.random.truncated_normal(jax.random.fold_in(key, 24), -6.0, 6.0, (MATS, TOK, FF)) * column_scale * matrix_scale
    return (0.25 * values).astype(jnp.bfloat16)


def draw_weights(key, part):
    row_scale = spread(jax.random.fold_in(key, 31), (MATS, D, 1), 0.2, 2.0) * rising(D, 1.7)[:, None]
    column_scale = spread(jax.random.fold_in(key, 32), (MATS, 1, FF), 0.2, 2.0) * rising(FF, 1.7)
    matrix_level = spread(jax.random.fold_in(key, 36), (MATS, 1, 1), 0.3, 3.0)
    values = jax.random.truncated_normal(jax.random.fold_in(key, 35), -6.0, 6.0, (MATS, D, FF)) * row_scale * column_scale
    return (values * matrix_level).astype(jnp.bfloat16)


def draw_state(key, length):
    matrix_level = spread(jax.random.fold_in(key, 41), (MATS, 1), 0.003, 0.3)
    entry_scale = spread(jax.random.fold_in(key, 43), (MATS, length), 0.3, 3.0)
    return (matrix_level * entry_scale).astype(jnp.float32)


def draw_row_state(key, part):
    return draw_state(jax.random.fold_in(key, 51), D)


def draw_col_state(key, part):
    return draw_state(jax.random.fold_in(key, 52), FF)


def setup_inputs(seed: int = 0) -> dict:
    splits = jax.random.split(jax.random.key(seed), 6)
    weights = draw_weights(jax.random.fold_in(splits[5], 71), 0)
    inputs = draw_inputs(jax.random.fold_in(splits[5], 71), 0)
    cotangents = draw_cotangents(jax.random.fold_in(splits[5], 71), 0)
    row_state = draw_row_state(jax.random.fold_in(splits[5], 71), 0)
    col_state = draw_col_state(jax.random.fold_in(splits[5], 71), 0)
    return dict(weights=weights, inputs=inputs, cotangents=cotangents, row_state=row_state, col_state=col_state)


eps_square = 1e-30

def gradient(matrix_inputs, matrix_cotangents):
    return jnp.dot(matrix_inputs.astype(jnp.float32).T, matrix_cotangents.astype(jnp.float32), preferred_element_type=jnp.float32)

def reference(weights, inputs, cotangents, row_state, col_state):
    gradients = lax.map(lambda operand_pair: gradient(operand_pair[0], operand_pair[1]), (inputs, cotangents))
    squared_total = jnp.sum(gradients * gradients)
    clip_scale = 1.0 / jnp.maximum(1.0, jnp.sqrt(squared_total / (MATS * D * FF)))
    decay_rate = 1.0 - STEP ** (-0.8)

    def update_one(operands):
        matrix_weights, matrix_grad, old_rows, old_cols = operands
        clipped = clip_scale * matrix_grad
        squares = clipped * clipped + eps_square
        new_rows = decay_rate * old_rows + (1.0 - decay_rate) * lax.optimization_barrier(jnp.mean(squares, axis=1))
        new_cols = decay_rate * old_cols + (1.0 - decay_rate) * lax.optimization_barrier(jnp.mean(squares, axis=0))
        row_average = jnp.mean(new_rows)
        second = new_rows[:, None] * new_cols[None, :] / row_average
        update = clipped / jnp.sqrt(second)
        update_rms = jnp.sqrt(jnp.mean(update * update))
        update = update / jnp.maximum(1.0, update_rms)
        weights_wide = matrix_weights.astype(jnp.float32)
        weight_rms = jnp.sqrt(jnp.mean(weights_wide * weights_wide))
        return (weight_rms * update, new_rows, new_cols)
    scaled_update, new_rows, new_cols = lax.map(update_one, (weights, gradients, row_state, col_state))
    return (scaled_update, new_rows, new_cols)
```

```python
import jax
import jax.numpy as jnp
from jax import lax
from jax.experimental import pallas as pl
from jax.experimental.pallas import tpu as pltpu
from jax.sharding import Mesh
from jax.sharding import PartitionSpec as P

STEP = 10
EPS = 1e-30
DECAY = 1.0 - STEP ** (-0.8)
EXPERT = ("ylo", "x", "core")
MESH = pl.DeviceIdType.MESH
F32 = jnp.float32
BF16 = jnp.bfloat16
SUBS = 4
LANES = 128
PLACE = (0, 1, 3, 2)


def neighbours():
    ylo, x, core = (lax.axis_index(a) for a in EXPERT)
    row, col = lax.axis_index("row"), lax.axis_index("col")
    group = []
    for dr in range(2):
        for dc in range(4):
            if dr or dc:
                place = {"row": lax.rem(row + dr, 2), "col": lax.rem(col + dc, 4)}
                group.append(((dr, dc), place))
    experts = []
    for dy in range(2):
        for dx in range(4):
            for dk in range(2):
                if dy or dx or dk:
                    place = {
                        "ylo": lax.rem(ylo + dy, 2),
                        "x": lax.rem(x + dx, 4),
                        "core": lax.rem(core + dk, 2),
                    }
                    experts.append(((dy, dx, dk), place))
    return dict(group), dict(experts)


def ring_sum(parts):
    return (parts[0] + parts[2]) + (parts[1] + parts[3])


def group_sum(parts):
    return ring_sum([parts[(0, c)] for c in range(4)]) + ring_sum([parts[(1, c)] for c in range(4)])


def full_sum(vector):
    return jnp.broadcast_to(jnp.sum(vector, keepdims=True), vector.shape)


def gather_kernel(
    weights, inputs, cotangents, row_state, col_state,
    grad, row_scale, col_scale, new_rows, new_cols,
    xg, yg, xt, xt_last, x_send, y_send, w_buf,
    w_acc, row_part, col_part, row_vec, col_vec, small,
    ring_rows, pair_cols, group_small, group_total, expert_total, update_part, group_update,
    local_sem, w_sem, yz_send, yz_recv, xz_send, xz_recv, fw_send, fw_recv, cross_send, cross_recv,
    r1_send, r1_recv, ex_send, ex_recv, r2_send, r2_recv,
):
    tokens = inputs.shape[1]
    rows, cols = grad.shape
    half, pair = rows // 2, 2 * tokens
    sub = half // SUBS
    row, col = lax.axis_index("row"), lax.axis_index("col")
    group, experts = neighbours()
    up, down, across = group[(0, 1)], group[(0, 3)], group[(0, 2)]
    partner = group[(1, 0)]

    def remote(src, dst, send, recv, device):
        return pltpu.make_async_remote_copy(
            src_ref=src, dst_ref=dst, send_sem=send, recv_sem=recv, device_id=device, device_id_type=MESH
        )

    def tokens_of(buffer, j, s, width=None):
        start = PLACE[j] * pair + s * tokens
        if width is None:
            return buffer.at[pl.ds(start, tokens)]
        return buffer.at[pl.ds(start, tokens), width]

    def row_cols(r):
        return pl.ds(pl.multiple_of(r * rows, rows), rows)

    def col_cols(c):
        return pl.ds(pl.multiple_of(c * cols, cols), cols)

    y_dest = (1, 3, 2)
    local = []
    for n, dc in enumerate(y_dest):
        local.append((cotangents.at[0, :, col_cols(lax.rem(col + dc, 4))], y_send.at[n]))
    local.append((inputs.at[0, :, row_cols(1 - row)], x_send))
    local.append((inputs.at[0, :, row_cols(row)], tokens_of(xg, 0, 0)))
    local.append((cotangents.at[0, :, col_cols(col)], tokens_of(yg, 0, 0)))
    loads = [pltpu.make_async_copy(s, d, local_sem.at[n]) for n, (s, d) in enumerate(local)]
    for n in (0, 1, 3, 4, 5, 2):
        loads[n].start()
    w_rows = w_buf.shape[1]
    w_steps = rows // w_rows

    def w_load(step, slot):
        start = pl.multiple_of(step * w_rows, w_rows)
        return pltpu.make_async_copy(weights.at[0, pl.ds(start, w_rows)], w_buf.at[slot], w_sem.at[slot])

    w_load(0, 0).start()

    barrier = pltpu.get_barrier_semaphore()
    everyone = [*group.values(), *experts.values()]
    for device in everyone:
        pl.semaphore_signal(barrier, inc=1, device_id=device, device_id_type=MESH)
    pl.semaphore_wait(barrier, len(everyone))

    y_copies = []
    for n, (dc, device) in enumerate(zip(y_dest, (up, down, across))):
        y_copies.append(
            remote(y_send.at[n], tokens_of(yg, (4 - dc) % 4, 0), yz_send.at[n], yz_recv.at[n], device)
        )
    lower, upper = pl.ds(0, half), pl.ds(half, half)

    def x_copy(s, direction, part):
        device, j = ((up, 3), (down, 1))[direction]
        width = (lower, upper)[direction ^ part]
        n = s * 4 + direction * 2 + part
        return remote(tokens_of(xg, 0, s, width), tokens_of(xg, j, s, width), xz_send.at[n], xz_recv.at[n], device)

    def forward(s, direction, step):
        device, j = ((up, 3), (down, 1))[direction]
        width = pl.ds(pl.multiple_of(direction * half + step * sub, LANES), sub)
        n = (s * 2 + direction) * SUBS + step
        return remote(tokens_of(xg, j, s, width), tokens_of(xg, 2, s, width), fw_send.at[n], fw_recv.at[n], device)

    cross_x = remote(x_send, tokens_of(xg, 0, 1), cross_send.at[4], cross_recv.at[4], partner)
    cross_y = [
        remote(tokens_of(yg, j, 0), tokens_of(yg, j, 1), cross_send.at[j], cross_recv.at[j], partner) for j in range(4)
    ]

    loads[0].wait()
    y_copies[0].start()
    loads[1].wait()
    y_copies[1].start()
    loads[3].wait()
    cross_x.start()
    loads[4].wait()
    for part in range(2):
        for direction in range(2):
            x_copy(0, direction, part).start()
    loads[5].wait()
    cross_y[0].start()
    loads[2].wait()
    y_copies[2].start()

    w_acc[...] = jnp.zeros_like(w_acc)

    @pl.loop(0, w_steps)
    def _(step):
        slot = lax.rem(step, 2)

        @pl.when(step + 1 < w_steps)
        def _():
            w_load(step + 1, 1 - slot).start()

        w_load(step, slot).wait()

        def add(i, total):
            block = w_buf[slot, pl.ds(pl.multiple_of(i * 16, 16), 16), :].astype(F32)
            block = block * block
            return total + (block[:8] + block[8:])

        w_acc[...] = lax.fori_loop(0, w_rows // 16, add, w_acc[...])

    weight_part = w_acc[:, :LANES]
    for n in range(1, cols // LANES):
        weight_part += w_acc[:, n * LANES : (n + 1) * LANES]
    small[8:16] = weight_part
    old_rows = row_state[...]
    small[16:24] = old_rows[:8] + old_rows[8:]

    def turn(first, count, start, width):
        @pl.loop(0, width // LANES)
        def _(i):
            at = pl.multiple_of(start + i * LANES, LANES)
            block = xg[first * pair : (first + count) * pair, pl.ds(at, LANES)]
            xt[pl.ds(at, LANES), first * pair : (first + count) * pair] = block.T

    n_width = 2 * LANES
    n_steps = cols // n_width

    def multiply(first, count, fresh):
        depth = slice(first * pair, (first + count) * pair)

        @pl.loop(0, n_steps)
        def _(n):
            at = pl.ds(pl.multiple_of(n * n_width, n_width), n_width)
            for m in range(2):
                part = jnp.dot(xt[m * half : (m + 1) * half, depth], yg[depth, at], preferred_element_type=F32)
                if not fresh:
                    part += grad[m * half : (m + 1) * half, at]
                grad[m * half : (m + 1) * half, at] = part

    y_copies[0].wait_recv()
    y_copies[1].wait_recv()
    cross_y[3].start()
    cross_y[1].start()
    cross_x.wait_recv()
    for part in range(2):
        for direction in range(2):
            x_copy(1, direction, part).start()
    turn(0, 1, 0, rows)
    cross_y[0].wait_recv()
    multiply(0, 1, True)
    y_copies[2].wait_recv()
    cross_y[2].start()

    for direction in range(2):
        x_copy(0, direction, 0).wait_recv()
    for direction in range(2):
        x_copy(1, direction, 0).wait_recv()
    for step in range(SUBS):
        for s in range(2):
            for direction in range(2):
                forward(s, direction, step).start()
    for s in range(2):
        for direction in range(2):
            x_copy(s, direction, 1).wait_recv()
    turn(1, 2, 0, rows)
    cross_y[3].wait_recv()
    cross_y[1].wait_recv()
    multiply(1, 2, False)
    cross_y[2].wait_recv()
    col_part[...] = jnp.zeros_like(col_part)

    last = slice(PLACE[2] * pair, (PLACE[2] + 1) * pair)

    @pl.loop(0, SUBS)
    def _(step):
        for s in range(2):
            for direction in range(2):
                forward(s, direction, step).wait_recv()
        starts = [pl.multiple_of(direction * half + step * sub, LANES) for direction in range(2)]
        for direction in range(2):
            for n in range(sub // LANES):
                at = pl.multiple_of(starts[direction] + n * LANES, LANES)
                to = direction * sub + n * LANES
                xt_last[to : to + LANES, :] = xg[last, pl.ds(at, LANES)].T
        row_part[...] = jnp.zeros_like(row_part)

        @pl.loop(0, n_steps)
        def _(n):
            at = pl.ds(pl.multiple_of(n * n_width, n_width), n_width)
            part = jnp.dot(xt_last[...], yg[last, at], preferred_element_type=F32)
            for direction in range(2):
                here = pl.ds(starts[direction], sub)
                block = part[direction * sub : (direction + 1) * sub] + grad[here, at]
                grad[here, at] = block
                block = block * block
                row_part[direction * sub : (direction + 1) * sub] += block[:, :LANES] + block[:, LANES:]
                col_part[:, at] += jnp.sum(block.reshape(sub // 8, 8, n_width), axis=0)

        for direction in range(2):
            for n in range(sub // LANES):
                to = direction * sub + n * LANES
                turned = row_part[to : to + LANES].T
                at = direction * (half // LANES) + step * (sub // LANES) + n
                row_vec[pl.ds(at, 1)] = jnp.sum(turned, axis=0, keepdims=True)

    col_vec[...] = jnp.sum(col_part[...], axis=0, keepdims=True)
    small[0:8] = row_vec[:8] + row_vec[8:]
    peers = list(group)
    r1 = []
    for dc in (1, 2, 3):
        r1.append(remote(row_vec, ring_rows.at[dc], r1_send.at[dc], r1_recv.at[dc], group[(0, (4 - dc) % 4)]))
    r1.append(remote(col_vec, pair_cols, r1_send.at[0], r1_recv.at[0], partner))
    for dr, dc in peers:
        n = dr * 4 + dc
        r1.append(
            remote(
                small, group_small.at[n], r1_send.at[4 + n], r1_recv.at[4 + n], group[(dr, (4 - dc) % 4)]
            )
        )
    for copy in r1[4:] + r1[:4]:
        copy.start()
    for copy in r1[4:]:
        copy.wait_recv()

    def of_group(part):
        parts = {(0, 0): small[part * 8 : part * 8 + 8]}
        for dr, dc in peers:
            parts[(dr, dc)] = group_small[dr * 4 + dc, part * 8 : part * 8 + 8]
        return parts

    squares = group_sum(of_group(0))
    group_total[...] = squares
    ex = []
    for n, (dy, dx, dk) in enumerate(experts):
        ex.append(
            remote(group_total, expert_total.at[n], ex_send.at[n], ex_recv.at[n], experts[(dy, (4 - dx) % 4, dk)])
        )
    for copy in ex:
        copy.start()
    weight_total = full_sum(group_sum(of_group(1)))
    old = of_group(2)
    old_total = full_sum(old[(0, 0)] + old[(1, 0)])
    group_squares = full_sum(squares)
    for copy in r1[:4]:
        copy.wait_recv()
    row_total = ring_sum([row_vec[...], ring_rows[1], ring_rows[2], ring_rows[3]])
    col_total = col_vec[...] + pair_cols[...]
    for copy in ex:
        copy.wait_recv()
    totals = {(0, 0, 0): squares}
    for n, key in enumerate(experts):
        totals[key] = expert_total[n]
    chips = [[totals[(dy, dx, 0)] + totals[(dy, dx, 1)] for dx in range(4)] for dy in range(2)]
    squared_total = full_sum(ring_sum(chips[0]) + ring_sum(chips[1]))

    model_width, hidden_width = 2 * rows, 4 * cols
    entries = model_width * hidden_width
    matrices = 1 + len(experts)
    clip = 1.0 / jnp.maximum(1.0, jnp.sqrt(squared_total / (matrices * entries)))
    clip_square = clip * clip
    row_square = jnp.concatenate([clip_square, clip_square], axis=0)
    fresh_rows = row_total * row_square + hidden_width * EPS
    fresh_cols = col_total * clip_square[:1, :1] + model_width * EPS
    rows_now = DECAY * row_state[...] + (1.0 - DECAY) * (fresh_rows / hidden_width)
    cols_now = DECAY * col_state[...] + (1.0 - DECAY) * (fresh_cols / model_width)
    new_rows[...] = rows_now
    new_cols[...] = cols_now
    average = DECAY * (old_total / model_width) + (1.0 - DECAY) * (group_squares * clip_square / entries + EPS)
    row_root = 1.0 / jnp.sqrt(rows_now)
    for n in range(rows // LANES):
        row_scale[n * LANES : (n + 1) * LANES] = jnp.broadcast_to(row_root[n : n + 1], (LANES, LANES)).T
    col_scale[...] = 1.0 / cols_now

    def weigh(i, total):
        here = pl.ds(pl.multiple_of(i * 32, 32), 32)
        line = None
        for n in range(cols // LANES):
            lane = slice(n * LANES, (n + 1) * LANES)
            block = grad[here, lane]
            block = block * block * col_scale[:, lane]
            line = block if line is None else line + block
        root = row_scale[here]
        line = line * root * root
        return total + ((line[0:8] + line[8:16]) + (line[16:24] + line[24:32]))

    update_part[...] = lax.fori_loop(0, rows // 32, weigh, jnp.zeros((8, LANES), F32))
    r2 = []
    for dr, dc in peers:
        n = dr * 4 + dc
        r2.append(
            remote(update_part, group_update.at[n], r2_send.at[n], r2_recv.at[n], group[(dr, (4 - dc) % 4)])
        )
    for copy in r2:
        copy.start()
    col_root = jnp.sqrt(col_scale[...])
    base = clip * jnp.sqrt(average) * jnp.sqrt(weight_total / entries)
    for copy in r2:
        copy.wait_recv()
    parts = {(0, 0): update_part[...]}
    for dr, dc in peers:
        parts[(dr, dc)] = group_update[dr * 4 + dc]
    update_total = full_sum(group_sum(parts)) * clip_square * average
    factor = base / jnp.maximum(1.0, jnp.sqrt(update_total / entries))
    col_scale[...] = col_root * factor[:1, :1]

    for copy in y_copies + [cross_x] + cross_y + r1 + ex + r2:
        copy.wait_send()
    for s in range(2):
        for direction in range(2):
            for part in range(2):
                x_copy(s, direction, part).wait_send()
            for step in range(SUBS):
                forward(s, direction, step).wait_send()


def scale_kernel(grad, row_scale, col_scale, rows_in, cols_in, out, rows_out, cols_out):
    step = pl.program_id(0)
    block = out.shape[0]

    @pl.when(step == 0)
    def _():
        rows_out[...] = rows_in[...]
        cols_out[...] = cols_in[...]

    @pl.loop(0, block // 8)
    def _(i):
        to = pl.ds(pl.multiple_of(i * 8, 8), 8)
        here = pl.ds(pl.multiple_of(step * block + i * 8, 8), 8)
        scale = row_scale[here]
        for n in range(out.shape[1] // LANES):
            lane = slice(n * LANES, (n + 1) * LANES)
            out[to, lane] = grad[here, lane] * scale * col_scale[:, lane]


def body(weights, inputs, cotangents, row_state, col_state):
    _, rows, cols = weights.shape
    tokens = inputs.shape[1]
    lines = rows // LANES
    vmem = pl.BlockSpec(memory_space=pltpu.VMEM)
    anywhere = pl.BlockSpec(memory_space=pl.ANY)
    shapes = [
        pltpu.VMEM((rows, cols), F32),
        pltpu.VMEM((rows, LANES), F32),
        pltpu.VMEM((1, cols), F32),
        pltpu.VMEM((lines, LANES), F32),
        pltpu.VMEM((1, cols), F32),
    ]
    sub = rows // 2 // SUBS
    dma = pltpu.SemaphoreType.DMA
    grad, row_scale, col_scale, new_rows, new_cols = pl.pallas_call(
        gather_kernel,
        name="gather_gradient",
        out_shape=shapes,
        in_specs=[anywhere, anywhere, anywhere, vmem, vmem],
        out_specs=[vmem] * 5,
        scratch_shapes=[
            pltpu.VMEM((8 * tokens, rows), BF16),
            pltpu.VMEM((8 * tokens, cols), BF16),
            pltpu.VMEM((rows, 6 * tokens), BF16),
            pltpu.VMEM((2 * sub, 2 * tokens), BF16),
            pltpu.VMEM((tokens, rows), BF16),
            pltpu.VMEM((3, tokens, cols), BF16),
            pltpu.VMEM((2, 256, cols), BF16),
            pltpu.VMEM((8, cols), F32),
            pltpu.VMEM((2 * sub, LANES), F32),
            pltpu.VMEM((8, cols), F32),
            pltpu.VMEM((lines, LANES), F32),
            pltpu.VMEM((1, cols), F32),
            pltpu.VMEM((24, LANES), F32),
            pltpu.VMEM((4, lines, LANES), F32),
            pltpu.VMEM((1, cols), F32),
            pltpu.VMEM((8, 24, LANES), F32),
            pltpu.VMEM((8, LANES), F32),
            pltpu.VMEM((15, 8, LANES), F32),
            pltpu.VMEM((8, LANES), F32),
            pltpu.VMEM((8, 8, LANES), F32),
            dma((6,)), dma((2,)), dma((3,)), dma((3,)), dma((8,)), dma((8,)),
            dma((4 * SUBS,)), dma((4 * SUBS,)), dma((5,)), dma((5,)),
            dma((12,)), dma((12,)), dma((15,)), dma((15,)), dma((8,)), dma((8,)),
        ],
        compiler_params=pltpu.CompilerParams(collective_id=0, has_side_effects=True, vmem_limit_bytes=44 * 2**20),
        cost_estimate=pl.CostEstimate(flops=16 * tokens * rows * cols, bytes_accessed=2**23, transcendentals=0),
    )(weights, inputs, cotangents, row_state.reshape(lines, LANES), col_state)
    steps = 8
    out, rows_out, cols_out = pl.pallas_call(
        scale_kernel,
        name="scale_update",
        grid=(steps,),
        out_shape=[
            jax.ShapeDtypeStruct((rows, cols), F32),
            jax.ShapeDtypeStruct((lines, LANES), F32),
            jax.ShapeDtypeStruct((1, cols), F32),
        ],
        in_specs=[vmem] * 5,
        out_specs=[
            pl.BlockSpec((rows // steps, cols), lambda i: (i, 0)),
            pl.BlockSpec((lines, LANES), lambda i: (0, 0)),
            pl.BlockSpec((1, cols), lambda i: (0, 0)),
        ],
        compiler_params=pltpu.CompilerParams(vmem_limit_bytes=10 * 2**20),
    )(grad, row_scale, col_scale, new_rows, new_cols)
    return out.reshape(1, rows, cols), rows_out.reshape(1, rows), cols_out


def solution(mesh):
    split = Mesh(
        mesh.devices.reshape(2, 4, 2, mesh.shape["row"], mesh.shape["col"]),
        (*EXPERT, "row", "col"),
    )
    return jax.shard_map(
        body,
        mesh=split,
        in_specs=(
            P(EXPERT, "row", "col"),
            P(EXPERT, ("row", "col"), None),
            P(EXPERT, ("row", "col"), None),
            P(EXPERT, "row"),
            P(EXPERT, "col"),
        ),
        out_specs=(P(EXPERT, "row", "col"), P(EXPERT, "row"), P(EXPERT, "col")),
        check_vma=False,
    )
```

```python
import jax
import jax.numpy as jnp
from jax import lax
from jax.experimental import pallas as pl
from jax.experimental.pallas import tpu as pltpu
from jax.sharding import Mesh
from jax.sharding import PartitionSpec as P

STEP = 10
EPS = 1e-30
DECAY = 1.0 - STEP ** (-0.8)
EXPERT = ("ylo", "x", "core")
MESH = pl.DeviceIdType.MESH
F32 = jnp.float32
BF16 = jnp.bfloat16
SUBS = 8
LANES = 128
PLACE = (0, 1, 3, 2)


def neighbours():
    ylo, x, core = (lax.axis_index(a) for a in EXPERT)
    row, col = lax.axis_index("row"), lax.axis_index("col")
    group = []
    for dr in range(2):
        for dc in range(4):
            if dr or dc:
                place = {"row": lax.rem(row + dr, 2), "col": lax.rem(col + dc, 4)}
                group.append(((dr, dc), place))
    experts = []
    for dy in range(2):
        for dx in range(4):
            for dk in range(2):
                if dy or dx or dk:
                    place = {
                        "ylo": lax.rem(ylo + dy, 2),
                        "x": lax.rem(x + dx, 4),
                        "core": lax.rem(core + dk, 2),
                    }
                    experts.append(((dy, dx, dk), place))
    return dict(group), dict(experts)


def ring_sum(parts):
    return (parts[0] + parts[2]) + (parts[1] + parts[3])


def group_sum(parts):
    return ring_sum([parts[(0, c)] for c in range(4)]) + ring_sum([parts[(1, c)] for c in range(4)])


def full_sum(vector):
    return jnp.broadcast_to(jnp.sum(vector, keepdims=True), vector.shape)


def gather_kernel(
    weights, inputs, cotangents, row_state_in, col_state_in,
    grad, row_scale, col_scale, new_rows, new_cols,
    xg, yg, xt, xt_last, x_send, y_send, w_buf, row_state, col_state,
    w_acc, squares, row_base, row_rate, row_part, col_part, row_vec, col_vec, small,
    ring_rows, pair_cols, group_small, group_total, expert_total, update_part, group_update,
    local_sem, w_sem, send_sem, yz_recv, xz_recv, fw_recv, cross_recv, sum_recv,
):
    tokens = inputs.shape[1]
    rows, cols = grad.shape
    half, pair = rows // 2, 2 * tokens
    sub = half // SUBS
    row, col = lax.axis_index("row"), lax.axis_index("col")
    group, experts = neighbours()
    up, down, across = group[(0, 1)], group[(0, 3)], group[(0, 2)]
    partner = group[(1, 0)]

    def remote(src, dst, send, recv, device):
        return pltpu.make_async_remote_copy(
            src_ref=src, dst_ref=dst, send_sem=send, recv_sem=recv, device_id=device, device_id_type=MESH
        )

    def tokens_of(buffer, j, s, width=None):
        start = PLACE[j] * pair + s * tokens
        if width is None:
            return buffer.at[pl.ds(start, tokens)]
        return buffer.at[pl.ds(start, tokens), width]

    def row_cols(r):
        return pl.ds(pl.multiple_of(r * rows, rows), rows)

    def col_cols(c):
        return pl.ds(pl.multiple_of(c * cols, cols), cols)

    y_dest = (1, 3, 2)
    local = []
    for n, dc in enumerate(y_dest):
        local.append((cotangents.at[0, :, col_cols(lax.rem(col + dc, 4))], y_send.at[n]))
    local.append((inputs.at[0, :, row_cols(1 - row)], x_send))
    local.append((inputs.at[0, :, row_cols(row)], tokens_of(xg, 0, 0)))
    local.append((cotangents.at[0, :, col_cols(col)], tokens_of(yg, 0, 0)))
    loads = [pltpu.make_async_copy(s, d, local_sem.at[n]) for n, (s, d) in enumerate(local)]
    loads.append(pltpu.make_async_copy(row_state_in, row_state, local_sem.at[6]))
    loads.append(pltpu.make_async_copy(col_state_in, col_state, local_sem.at[7]))
    for n in (0, 1, 3, 4, 5, 2, 6, 7):
        loads[n].start()
    w_rows = w_buf.shape[1]
    w_steps = rows // w_rows

    def w_load(step, slot):
        start = pl.multiple_of(step * w_rows, w_rows)
        return pltpu.make_async_copy(weights.at[0, pl.ds(start, w_rows)], w_buf.at[slot], w_sem.at[slot])

    w_load(0, 0).start()

    barrier = pltpu.get_barrier_semaphore()
    everyone = [*group.values(), *experts.values()]
    for device in everyone:
        pl.semaphore_signal(barrier, inc=1, device_id=device, device_id_type=MESH)
    pl.semaphore_wait(barrier, len(everyone))

    y_copies = []
    for n, (dc, device) in enumerate(zip(y_dest, (up, down, across))):
        y_copies.append(
            remote(y_send.at[n], tokens_of(yg, (4 - dc) % 4, 0), send_sem.at[0], yz_recv.at[n], device)
        )
    lower, upper = pl.ds(0, half), pl.ds(half, half)

    def x_copy(s, direction, part):
        device, j = ((up, 3), (down, 1))[direction]
        width = (lower, upper)[direction ^ part]
        recv = xz_recv.at[s * 2 + part]
        return remote(tokens_of(xg, 0, s, width), tokens_of(xg, j, s, width), send_sem.at[1], recv, device)

    def forward(s, direction, step):
        device, j = ((up, 3), (down, 1))[direction]
        width = pl.ds(direction * half + step * sub, sub)
        return remote(
            tokens_of(xg, j, s, width), tokens_of(xg, 2, s, width), send_sem.at[2], fw_recv.at[step], device
        )

    def await_bytes(like, sem):
        pltpu.make_async_copy(like, like, sem).wait()

    cross_x = remote(x_send, tokens_of(xg, 0, 1), send_sem.at[3], cross_recv.at[4], partner)
    cross_y = [
        remote(tokens_of(yg, j, 0), tokens_of(yg, j, 1), send_sem.at[4], cross_recv.at[j], partner) for j in range(4)
    ]

    loads[0].wait()
    y_copies[0].start()
    loads[1].wait()
    y_copies[1].start()
    loads[3].wait()
    cross_x.start()
    loads[4].wait()
    for part in range(2):
        for direction in range(2):
            x_copy(0, direction, part).start()
    loads[5].wait()
    cross_y[0].start()
    loads[2].wait()
    y_copies[2].start()

    w_acc[...] = jnp.zeros_like(w_acc)

    @pl.loop(0, w_steps)
    def _(step):
        slot = lax.rem(step, 2)

        @pl.when(step + 1 < w_steps)
        def _():
            w_load(step + 1, 1 - slot).start()

        w_load(step, slot).wait()

        def add(i, total):
            block = w_buf[slot, pl.ds(pl.multiple_of(i * 16, 16), 16), :].astype(F32)
            block = block * block
            return total + (block[:8] + block[8:])

        w_acc[...] = lax.fori_loop(0, w_rows // 16, add, w_acc[...])

    weight_part = w_acc[:, :LANES]
    for n in range(1, cols // LANES):
        weight_part += w_acc[:, n * LANES : (n + 1) * LANES]
    small[8:16] = weight_part
    loads[6].wait()
    loads[7].wait()
    old_rows = row_state[...]
    small[16:24] = old_rows[:8] + old_rows[8:]

    def turn(first, count, start, width):
        @pl.loop(0, width // LANES)
        def _(i):
            at = pl.multiple_of(start + i * LANES, LANES)
            block = xg[first * pair : (first + count) * pair, pl.ds(at, LANES)]
            xt[pl.ds(at, LANES), first * pair : (first + count) * pair] = block.T

    n_width = 2 * LANES
    n_steps = cols // n_width

    def multiply(place, halves, fresh=False):
        depth = slice(place * pair, (place + 1) * pair)

        @pl.loop(0, n_steps)
        def _(n):
            at = pl.ds(pl.multiple_of(n * n_width, n_width), n_width)
            for m in halves:
                here = slice(m * half, (m + 1) * half)
                part = jnp.dot(xt[here, depth], yg[depth, at], preferred_element_type=F32)
                if not fresh:
                    part += grad[here, at]
                grad[here, at] = part

    y_copies[0].wait_recv()
    y_copies[1].wait_recv()
    cross_y[3].start()
    cross_y[1].start()
    cross_x.wait_recv()
    for part in range(2):
        for direction in range(2):
            x_copy(1, direction, part).start()
    turn(0, 1, 0, rows)
    cross_y[0].wait_recv()
    multiply(0, (0, 1), fresh=True)
    y_copies[2].wait_recv()
    cross_y[2].start()

    await_bytes(x_send, xz_recv.at[0])
    await_bytes(x_send, xz_recv.at[2])
    for step in range(SUBS):
        for s in range(2):
            for direction in range(2):
                forward(s, direction, step).start()
    turn(2, 1, 0, half)
    turn(1, 1, half, half)
    cross_y[3].wait_recv()
    multiply(2, (0,))
    cross_y[1].wait_recv()
    multiply(1, (1,))
    await_bytes(x_send, xz_recv.at[1])
    await_bytes(x_send, xz_recv.at[3])
    turn(2, 1, half, half)
    turn(1, 1, 0, half)
    multiply(2, (1,))
    multiply(1, (0,))
    cross_y[2].wait_recv()
    col_part[...] = jnp.zeros_like(col_part)

    last = slice(PLACE[2] * pair, (PLACE[2] + 1) * pair)
    lanes = [slice(n * LANES, (n + 1) * LANES) for n in range(cols // LANES)]

    def finish(begin, width):
        starts = [pl.multiple_of(direction * half + begin, LANES) for direction in range(2)]
        for direction in range(2):
            for n in range(width // LANES):
                at = pl.multiple_of(starts[direction] + n * LANES, LANES)
                to = direction * width + n * LANES
                xt_last[to : to + LANES, :] = xg[last, pl.ds(at, LANES)].T

        @pl.loop(0, n_steps)
        def _(n):
            at = pl.ds(pl.multiple_of(n * n_width, n_width), n_width)
            part = jnp.dot(xt_last[: 2 * width], yg[last, at], preferred_element_type=F32)
            for direction in range(2):
                here = pl.ds(starts[direction], width)
                grad[here, at] = part[direction * width : (direction + 1) * width] + grad[here, at]

        for direction in range(2):

            def add(i, total):
                here = pl.ds(pl.multiple_of(starts[direction] + i * 8, 8), 8)
                line, out = None, []
                for lane, so_far in zip(lanes, total):
                    block = grad[here, lane]
                    block = block * block
                    squares[here, lane] = block
                    line = block if line is None else line + block
                    out.append(so_far + block)
                row_part[pl.ds(pl.multiple_of(direction * width + i * 8, 8), 8)] = line
                return tuple(out)

            total = lax.fori_loop(0, width // 8, add, tuple(col_part[:, lane] for lane in lanes), unroll=4)
            for lane, so_far in zip(lanes, total):
                col_part[:, lane] = so_far
            for n in range(width // LANES):
                to = direction * width + n * LANES
                turned = row_part[to : to + LANES].T
                at = (starts[direction] + n * LANES) // LANES
                row_vec[pl.ds(at, 1)] = jnp.sum(turned, axis=0, keepdims=True)

    def await_forward(step):
        await_bytes(x_send.at[:, pl.ds(0, 4 * sub)], fw_recv.at[step])

    double = SUBS // 2 - 1

    @pl.loop(0, double)
    def _(step):
        await_forward(2 * step)
        await_forward(2 * step + 1)
        finish(2 * step * sub, 2 * sub)

    @pl.loop(2 * double, SUBS)
    def _(step):
        await_forward(step)
        finish(step * sub, sub)

    col_vec[...] = jnp.sum(col_part[...], axis=0, keepdims=True)
    small[0:8] = row_vec[:8] + row_vec[8:]
    peers = list(group)
    for dr, dc in peers:
        n = dr * 4 + dc - 1
        remote(small, group_small.at[n], send_sem.at[5], sum_recv.at[0], group[(dr, (4 - dc) % 4)]).start()
    for dc in (1, 2, 3):
        remote(row_vec, ring_rows.at[dc - 1], send_sem.at[6], sum_recv.at[1], group[(0, (4 - dc) % 4)]).start()
    pair_copy = remote(col_vec, pair_cols, send_sem.at[7], sum_recv.at[2], partner)
    pair_copy.start()
    await_bytes(group_small, sum_recv.at[0])

    def of_group(part):
        parts = {(0, 0): small[part * 8 : part * 8 + 8]}
        for dr, dc in peers:
            parts[(dr, dc)] = group_small[dr * 4 + dc - 1, part * 8 : part * 8 + 8]
        return parts

    square_part = group_sum(of_group(0))
    group_total[...] = square_part
    for n, (dy, dx, dk) in enumerate(experts):
        remote(
            group_total, expert_total.at[n], send_sem.at[8], sum_recv.at[3], experts[(dy, (4 - dx) % 4, dk)]
        ).start()
    model_width, hidden_width = 2 * rows, 4 * cols
    entries = model_width * hidden_width
    matrices = 1 + len(experts)
    weight_total = full_sum(group_sum(of_group(1)))
    old = of_group(2)
    old_total = full_sum(old[(0, 0)] + old[(1, 0)])
    group_squares = full_sum(square_part)
    await_bytes(ring_rows, sum_recv.at[1])
    pair_copy.wait_recv()
    row_total = ring_sum([row_vec[...], ring_rows[0], ring_rows[1], ring_rows[2]])
    col_total = col_vec[...] + pair_cols[...]
    base = DECAY * row_state[...] + (1.0 - DECAY) * EPS
    rate = (1.0 - DECAY) * (row_total / hidden_width)
    for n in range(rows // LANES):
        here = slice(n * LANES, (n + 1) * LANES)
        row_base[here] = jnp.broadcast_to(base[n : n + 1], (LANES, LANES)).T
        row_rate[here] = jnp.broadcast_to(rate[n : n + 1], (LANES, LANES)).T
    await_bytes(expert_total, sum_recv.at[3])
    totals = {(0, 0, 0): square_part}
    for n, key in enumerate(experts):
        totals[key] = expert_total[n]
    chips = [[totals[(dy, dx, 0)] + totals[(dy, dx, 1)] for dx in range(4)] for dy in range(2)]
    squared_total = full_sum(ring_sum(chips[0]) + ring_sum(chips[1]))
    clip = 1.0 / jnp.maximum(1.0, jnp.sqrt(squared_total / (matrices * entries)))
    clip_square = clip * clip
    one = clip_square[:1, :1]
    fresh_cols = col_total * one + model_width * EPS
    cols_now = DECAY * col_state[...] + (1.0 - DECAY) * (fresh_cols / model_width)
    col_scale[...] = 1.0 / cols_now

    def weigh(i, total):
        here = pl.ds(pl.multiple_of(i * 64, 64), 64)
        line = None
        for lane in lanes:
            block = squares[here, lane] * col_scale[:, lane]
            line = block if line is None else line + block
        line = line / (row_base[here] + row_rate[here] * one)
        return total + jnp.sum(line.reshape(8, 8, LANES), axis=0)

    update_part[...] = lax.fori_loop(0, rows // 64, weigh, jnp.zeros((8, LANES), F32))
    for dr, dc in peers:
        n = dr * 4 + dc - 1
        remote(update_part, group_update.at[n], send_sem.at[9], sum_recv.at[4], group[(dr, (4 - dc) % 4)]).start()
    new_rows[...] = base + rate * one
    new_cols[...] = cols_now
    average = DECAY * (old_total / model_width) + (1.0 - DECAY) * (group_squares * clip_square / entries + EPS)

    @pl.loop(0, rows // 64)
    def _(i):
        here = pl.ds(pl.multiple_of(i * 64, 64), 64)
        row_scale[here] = 1.0 / jnp.sqrt(row_base[here] + row_rate[here] * one)

    col_root = jnp.sqrt(col_scale[...])
    scale = clip * jnp.sqrt(average) * jnp.sqrt(weight_total / entries)
    await_bytes(y_send, send_sem.at[0])
    await_bytes(xg.at[pl.ds(0, 4 * tokens)], send_sem.at[1])
    await_bytes(xg.at[pl.ds(0, 2 * tokens)], send_sem.at[2])
    cross_x.wait_send()
    await_bytes(yg.at[pl.ds(0, 4 * tokens)], send_sem.at[4])
    await_bytes(group_small, send_sem.at[5])
    await_bytes(ring_rows, send_sem.at[6])
    pair_copy.wait_send()
    await_bytes(expert_total, send_sem.at[8])
    await_bytes(group_update, send_sem.at[9])
    await_bytes(group_update, sum_recv.at[4])
    parts = {(0, 0): update_part[...]}
    for dr, dc in peers:
        parts[(dr, dc)] = group_update[dr * 4 + dc - 1]
    update_total = full_sum(group_sum(parts)) * clip_square * average
    factor = scale / jnp.maximum(1.0, jnp.sqrt(update_total / entries))
    col_scale[...] = col_root * factor[:1, :1]


def scale_kernel(grad, row_scale, col_scale, rows_in, cols_in, out, rows_out, cols_out, scaled, sem):
    rows, cols = grad.shape
    height = 64
    rows_copy = pltpu.make_async_copy(rows_in, rows_out, sem.at[1])
    cols_copy = pltpu.make_async_copy(cols_in, cols_out, sem.at[2])
    rows_copy.start()
    cols_copy.start()

    @pl.loop(0, rows // height)
    def _(step):
        for i in range(height // 8):
            here = pl.ds(pl.multiple_of(step * height + i * 8, 8), 8)
            scale = row_scale[here]
            for n in range(cols // LANES):
                lane = slice(n * LANES, (n + 1) * LANES)
                scaled[here, lane] = grad[here, lane] * scale * col_scale[:, lane]
        block = pl.ds(pl.multiple_of(step * height, height), height)
        pltpu.make_async_copy(scaled.at[block], out.at[block], sem.at[0]).start()

    rows_copy.wait()
    cols_copy.wait()
    pltpu.make_async_copy(scaled, out, sem.at[0]).wait()


def body(weights, inputs, cotangents, row_state, col_state):
    _, rows, cols = weights.shape
    tokens = inputs.shape[1]
    lines = rows // LANES
    vmem = pl.BlockSpec(memory_space=pltpu.VMEM)
    anywhere = pl.BlockSpec(memory_space=pl.ANY)
    shapes = [
        pltpu.VMEM((rows, cols), F32),
        pltpu.VMEM((rows, LANES), F32),
        pltpu.VMEM((1, cols), F32),
        pltpu.VMEM((lines, LANES), F32),
        pltpu.VMEM((1, cols), F32),
    ]
    sub = rows // 2 // SUBS
    dma = pltpu.SemaphoreType.DMA
    grad, row_scale, col_scale, new_rows, new_cols = pl.pallas_call(
        gather_kernel,
        name="gather_gradient",
        out_shape=shapes,
        in_specs=[anywhere] * 5,
        out_specs=[vmem] * 5,
        scratch_shapes=[
            pltpu.VMEM((8 * tokens, rows), BF16),
            pltpu.VMEM((8 * tokens, cols), BF16),
            pltpu.VMEM((rows, 6 * tokens), BF16),
            pltpu.VMEM((4 * sub, 2 * tokens), BF16),
            pltpu.VMEM((tokens, rows), BF16),
            pltpu.VMEM((3, tokens, cols), BF16),
            pltpu.VMEM((2, 256, cols), BF16),
            pltpu.VMEM((lines, LANES), F32),
            pltpu.VMEM((1, cols), F32),
            pltpu.VMEM((8, cols), F32),
            pltpu.VMEM((rows, cols), F32),
            pltpu.VMEM((rows, LANES), F32),
            pltpu.VMEM((rows, LANES), F32),
            pltpu.VMEM((4 * sub, LANES), F32),
            pltpu.VMEM((8, cols), F32),
            pltpu.VMEM((lines, LANES), F32),
            pltpu.VMEM((1, cols), F32),
            pltpu.VMEM((24, LANES), F32),
            pltpu.VMEM((3, lines, LANES), F32),
            pltpu.VMEM((1, cols), F32),
            pltpu.VMEM((7, 24, LANES), F32),
            pltpu.VMEM((8, LANES), F32),
            pltpu.VMEM((15, 8, LANES), F32),
            pltpu.VMEM((8, LANES), F32),
            pltpu.VMEM((7, 8, LANES), F32),
            dma((8,)), dma((2,)), dma((10,)), dma((3,)), dma((4,)), dma((SUBS,)), dma((5,)), dma((5,)),
        ],
        compiler_params=pltpu.CompilerParams(collective_id=0, has_side_effects=True, vmem_limit_bytes=40 * 2**20),
        cost_estimate=pl.CostEstimate(flops=16 * tokens * rows * cols, bytes_accessed=2**23, transcendentals=0),
    )(weights, inputs, cotangents, row_state.reshape(lines, LANES), col_state)
    out, rows_out, cols_out = pl.pallas_call(
        scale_kernel,
        name="scale_update",
        out_shape=[
            jax.ShapeDtypeStruct((rows, cols), F32),
            jax.ShapeDtypeStruct((lines, LANES), F32),
            jax.ShapeDtypeStruct((1, cols), F32),
        ],
        in_specs=[vmem] * 5,
        out_specs=[anywhere] * 3,
        scratch_shapes=[pltpu.VMEM((rows, cols), F32), dma((3,))],
        compiler_params=pltpu.CompilerParams(vmem_limit_bytes=20 * 2**20),
    )(grad, row_scale, col_scale, new_rows, new_cols)
    return out.reshape(1, rows, cols), rows_out.reshape(1, rows), cols_out


def solution(mesh):
    split = Mesh(
        mesh.devices.reshape(2, 4, 2, mesh.shape["row"], mesh.shape["col"]),
        (*EXPERT, "row", "col"),
    )
    return jax.shard_map(
        body,
        mesh=split,
        in_specs=(
            P(EXPERT, "row", "col"),
            P(EXPERT, ("row", "col"), None),
            P(EXPERT, ("row", "col"), None),
            P(EXPERT, "row"),
            P(EXPERT, "col"),
        ),
        out_specs=(P(EXPERT, "row", "col"), P(EXPERT, "row"), P(EXPERT, "col")),
        check_vma=False,
    )
```

```python
import jax
import jax.numpy as jnp
from jax import lax
from jax.experimental import pallas as pl
from jax.experimental.pallas import tpu as pltpu
from jax.sharding import Mesh
from jax.sharding import PartitionSpec as P

STEP = 10
EPS = 1e-30
DECAY = 1.0 - STEP ** (-0.8)
EXPERT = ("ylo", "x", "core")
MESH = pl.DeviceIdType.MESH
F32 = jnp.float32
BF16 = jnp.bfloat16
SUBS = 8
LANES = 128
LAST_STEPS = ((0, 3), (3, 6), (6, 7))
PLACE = (0, 1, 3, 2)


def neighbours():
    ylo, x, core = (lax.axis_index(a) for a in EXPERT)
    row, col = lax.axis_index("row"), lax.axis_index("col")
    group = []
    for dr in range(2):
        for dc in range(4):
            if dr or dc:
                place = {"row": lax.rem(row + dr, 2), "col": lax.rem(col + dc, 4)}
                group.append(((dr, dc), place))
    experts = []
    for dy in range(2):
        for dx in range(4):
            for dk in range(2):
                if dy or dx or dk:
                    place = {
                        "ylo": lax.rem(ylo + dy, 2),
                        "x": lax.rem(x + dx, 4),
                        "core": lax.rem(core + dk, 2),
                    }
                    experts.append(((dy, dx, dk), place))
    return dict(group), dict(experts)


def ring_sum(parts):
    return (parts[0] + parts[2]) + (parts[1] + parts[3])


def group_sum(parts):
    return ring_sum([parts[(0, c)] for c in range(4)]) + ring_sum([parts[(1, c)] for c in range(4)])


def full_sum(vector):
    return jnp.broadcast_to(jnp.sum(vector, keepdims=True), vector.shape)


def gather_kernel(
    weights, inputs, cotangents, row_state_in, col_state_in,
    grad, row_scale, col_scale, new_rows, new_cols,
    xg, yg, xt, xt_last, x_send, y_send, w_buf, row_state, col_state,
    w_acc, squares, row_base, row_rate, row_part, col_part, row_vec, col_vec, small,
    ring_rows, pair_cols, group_small, group_total, expert_total, update_part, group_update,
    local_sem, w_sem, send_sem, yz_recv, xz_recv, fw_recv, cross_recv, sum_recv,
):
    tokens = inputs.shape[1]
    rows, cols = grad.shape
    half, pair = rows // 2, 2 * tokens
    sub = half // SUBS
    row, col = lax.axis_index("row"), lax.axis_index("col")
    group, experts = neighbours()
    up, down, across = group[(0, 1)], group[(0, 3)], group[(0, 2)]
    partner = group[(1, 0)]

    def remote(src, dst, send, recv, device):
        return pltpu.make_async_remote_copy(
            src_ref=src, dst_ref=dst, send_sem=send, recv_sem=recv, device_id=device, device_id_type=MESH
        )

    def tokens_of(buffer, j, s, width=None):
        start = PLACE[j] * pair + s * tokens
        if width is None:
            return buffer.at[pl.ds(start, tokens)]
        return buffer.at[pl.ds(start, tokens), width]

    def row_cols(r):
        return pl.ds(pl.multiple_of(r * rows, rows), rows)

    def col_cols(c):
        return pl.ds(pl.multiple_of(c * cols, cols), cols)

    y_dest = (1, 3, 2)
    local = []
    for n, dc in enumerate(y_dest):
        local.append((cotangents.at[0, :, col_cols(lax.rem(col + dc, 4))], y_send.at[n]))
    local.append((inputs.at[0, :, row_cols(1 - row)], x_send))
    local.append((inputs.at[0, :, row_cols(row)], tokens_of(xg, 0, 0)))
    local.append((cotangents.at[0, :, col_cols(col)], tokens_of(yg, 0, 0)))
    loads = [pltpu.make_async_copy(s, d, local_sem.at[n]) for n, (s, d) in enumerate(local)]
    loads.append(pltpu.make_async_copy(row_state_in, row_state, local_sem.at[6]))
    loads.append(pltpu.make_async_copy(col_state_in, col_state, local_sem.at[7]))
    for n in (0, 1, 3, 4, 5, 2, 6, 7):
        loads[n].start()
    w_rows = w_buf.shape[1]
    w_steps = rows // w_rows

    def w_load(step, slot):
        start = pl.multiple_of(step * w_rows, w_rows)
        return pltpu.make_async_copy(weights.at[0, pl.ds(start, w_rows)], w_buf.at[slot], w_sem.at[slot])

    w_load(0, 0).start()

    barrier = pltpu.get_barrier_semaphore()
    everyone = [*group.values(), *experts.values()]
    for device in everyone:
        pl.semaphore_signal(barrier, inc=1, device_id=device, device_id_type=MESH)
    pl.semaphore_wait(barrier, len(everyone))

    y_copies = []
    for n, (dc, device) in enumerate(zip(y_dest, (up, down, across))):
        y_copies.append(
            remote(y_send.at[n], tokens_of(yg, (4 - dc) % 4, 0), send_sem.at[0], yz_recv.at[n], device)
        )
    lower, upper = pl.ds(0, half), pl.ds(half, half)

    def x_copy(s, direction, part):
        device, j = ((up, 3), (down, 1))[direction]
        width = (lower, upper)[direction ^ part]
        recv = xz_recv.at[s * 2 + part]
        return remote(tokens_of(xg, 0, s, width), tokens_of(xg, j, s, width), send_sem.at[1], recv, device)

    def forward(s, direction, step):
        device, j = ((up, 3), (down, 1))[direction]
        width = pl.ds(direction * half + step * sub, sub)
        return remote(
            tokens_of(xg, j, s, width), tokens_of(xg, 2, s, width), send_sem.at[2], fw_recv.at[step], device
        )

    def await_bytes(like, sem):
        pltpu.make_async_copy(like, like, sem).wait()

    cross_x = remote(x_send, tokens_of(xg, 0, 1), send_sem.at[3], cross_recv.at[4], partner)
    cross_y = {
        j: remote(tokens_of(yg, j, 0), tokens_of(yg, j, 1), send_sem.at[4], cross_recv.at[j], partner) for j in (0, 1, 3)
    }
    n_width = 2 * LANES
    n_steps = cols // n_width
    cross_last = []
    for n, (first, end) in enumerate(LAST_STEPS):
        width = pl.ds(first * n_width, (end - first) * n_width)
        recv = cross_recv.at[5 + n]
        cross_last.append(remote(tokens_of(yg, 2, 0, width), tokens_of(yg, 2, 1, width), send_sem.at[4], recv, partner))

    loads[0].wait()
    y_copies[0].start()
    loads[1].wait()
    y_copies[1].start()
    loads[3].wait()
    cross_x.start()
    loads[4].wait()
    for part in range(2):
        for direction in range(2):
            x_copy(0, direction, part).start()
    loads[5].wait()
    cross_y[0].start()
    loads[2].wait()
    y_copies[2].start()

    w_acc[...] = jnp.zeros_like(w_acc)

    @pl.loop(0, w_steps)
    def _(step):
        slot = lax.rem(step, 2)

        @pl.when(step + 1 < w_steps)
        def _():
            w_load(step + 1, 1 - slot).start()

        w_load(step, slot).wait()

        def add(i, total):
            block = w_buf[slot, pl.ds(pl.multiple_of(i * 16, 16), 16), :].astype(F32)
            block = block * block
            return total + (block[:8] + block[8:])

        w_acc[...] = lax.fori_loop(0, w_rows // 16, add, w_acc[...])

    weight_part = w_acc[:, :LANES]
    for n in range(1, cols // LANES):
        weight_part += w_acc[:, n * LANES : (n + 1) * LANES]
    small[8:16] = weight_part
    loads[6].wait()
    loads[7].wait()
    old_rows = row_state[...]
    small[16:24] = old_rows[:8] + old_rows[8:]

    def turn(first, count, start, width):
        @pl.loop(0, width // LANES)
        def _(i):
            at = pl.multiple_of(start + i * LANES, LANES)
            block = xg[first * pair : (first + count) * pair, pl.ds(at, LANES)]
            xt[pl.ds(at, LANES), first * pair : (first + count) * pair] = block.T

    def multiply(place, halves, fresh=False):
        depth = slice(place * pair, (place + 1) * pair)

        for n in range(n_steps):
            at = slice(n * n_width, (n + 1) * n_width)
            for m in halves:
                here = slice(m * half, (m + 1) * half)
                part = jnp.dot(xt[here, depth], yg[depth, at], preferred_element_type=F32)
                if not fresh:
                    part += grad[here, at]
                grad[here, at] = part

    y_copies[0].wait_recv()
    y_copies[1].wait_recv()
    cross_y[3].start()
    cross_y[1].start()
    cross_x.wait_recv()
    for part in range(2):
        for direction in range(2):
            x_copy(1, direction, part).start()
    turn(0, 1, 0, rows)
    cross_y[0].wait_recv()
    multiply(0, (0, 1), fresh=True)
    y_copies[2].wait_recv()
    for copy in cross_last:
        copy.start()

    await_bytes(x_send, xz_recv.at[0])
    await_bytes(x_send, xz_recv.at[2])
    for step in range(SUBS):
        for s in range(2):
            for direction in range(2):
                forward(s, direction, step).start()
    turn(2, 1, 0, half)
    turn(1, 1, half, half)
    cross_y[3].wait_recv()
    multiply(2, (0,))
    cross_y[1].wait_recv()
    multiply(1, (1,))
    await_bytes(x_send, xz_recv.at[1])
    await_bytes(x_send, xz_recv.at[3])
    turn(2, 1, half, half)
    turn(1, 1, 0, half)
    multiply(2, (1,))
    multiply(1, (0,))
    col_part[...] = jnp.zeros_like(col_part)
    last = slice(PLACE[2] * pair, (PLACE[2] + 1) * pair)
    lanes = [slice(n * LANES, (n + 1) * LANES) for n in range(cols // LANES)]

    def await_forward(step):
        await_bytes(x_send.at[:, pl.ds(0, 4 * sub)], fw_recv.at[step])
        for direction in range(2):
            at = direction * half + step * sub
            to = (2 * step + direction) * sub
            xt_last[to : to + sub, :] = xg[last, at : at + sub].T

    def finish(first, end, steps):
        for n in range(*steps):
            at = slice(n * n_width, (n + 1) * n_width)
            part = jnp.dot(xt_last[first * 2 * sub : end * 2 * sub], yg[last, at], preferred_element_type=F32)
            total = col_part[:, at]
            for step in range(first, end):
                for direction in range(2):
                    here = slice(direction * half + step * sub, direction * half + (step + 1) * sub)
                    begin = (2 * (step - first) + direction) * sub
                    block = part[begin : begin + sub] + grad[here, at]
                    grad[here, at] = block
                    block = block * block
                    total += jnp.sum(block.reshape(sub // 8, 8, n_width), axis=0)
            col_part[:, at] = total

    def square(first, width):
        for direction in range(2):

            @pl.loop(0, width // 32)
            def _(i):
                for k in range(4):
                    begin = direction * half + first + i * 32 + k * 8
                    here = pl.ds(pl.multiple_of(begin, 8), 8)
                    line = None
                    for lane in lanes:
                        block = grad[here, lane]
                        block = block * block
                        squares[here, lane] = block
                        line = block if line is None else line + block
                    row_part[here] = line

            for n in range(width // LANES):
                begin = direction * half + first + n * LANES
                turned = row_part[begin : begin + LANES].T
                row_vec[begin // LANES : begin // LANES + 1] = jnp.sum(turned, axis=0, keepdims=True)

    await_forward(0)
    await_forward(1)
    cross_last[0].wait_recv()
    finish(0, 2, LAST_STEPS[0])
    await_forward(2)
    await_forward(3)
    finish(2, 4, LAST_STEPS[0])
    cross_last[1].wait_recv()
    finish(0, 4, LAST_STEPS[1])
    await_forward(4)
    await_forward(5)
    finish(4, 6, (0, LAST_STEPS[1][1]))
    cross_last[2].wait_recv()
    finish(0, 6, LAST_STEPS[2])
    await_forward(6)
    finish(6, 7, (0, n_steps))
    square(0, 2 * sub)
    await_forward(7)
    finish(7, 8, (0, n_steps))

    square_part = col_part[:, :LANES]
    for lane in lanes[1:]:
        square_part += col_part[:, lane]
    small[0:8] = square_part
    peers = list(group)
    for dr, dc in peers:
        n = dr * 4 + dc - 1
        remote(small, group_small.at[n], send_sem.at[5], sum_recv.at[0], group[(dr, (4 - dc) % 4)]).start()
    col_vec[...] = jnp.sum(col_part[...], axis=0, keepdims=True)
    square(2 * sub, 6 * sub)
    for dc in (1, 2, 3):
        remote(row_vec, ring_rows.at[dc - 1], send_sem.at[6], sum_recv.at[1], group[(0, (4 - dc) % 4)]).start()
    pair_copy = remote(col_vec, pair_cols, send_sem.at[7], sum_recv.at[2], partner)
    pair_copy.start()
    await_bytes(group_small, sum_recv.at[0])

    def of_group(part):
        parts = {(0, 0): small[part * 8 : part * 8 + 8]}
        for dr, dc in peers:
            parts[(dr, dc)] = group_small[dr * 4 + dc - 1, part * 8 : part * 8 + 8]
        return parts

    square_part = group_sum(of_group(0))
    group_total[...] = square_part
    for n, (dy, dx, dk) in enumerate(experts):
        remote(
            group_total, expert_total.at[n], send_sem.at[8], sum_recv.at[3], experts[(dy, (4 - dx) % 4, dk)]
        ).start()
    model_width, hidden_width = 2 * rows, 4 * cols
    entries = model_width * hidden_width
    matrices = 1 + len(experts)
    weight_total = full_sum(group_sum(of_group(1)))
    old = of_group(2)
    old_total = full_sum(old[(0, 0)] + old[(1, 0)])
    group_squares = full_sum(square_part)
    await_bytes(ring_rows, sum_recv.at[1])
    pair_copy.wait_recv()
    row_total = ring_sum([row_vec[...], ring_rows[0], ring_rows[1], ring_rows[2]])
    col_total = col_vec[...] + pair_cols[...]
    base = DECAY * row_state[...] + (1.0 - DECAY) * EPS
    rate = (1.0 - DECAY) * (row_total / hidden_width)
    for n in range(rows // LANES):
        here = slice(n * LANES, (n + 1) * LANES)
        row_base[here] = jnp.broadcast_to(base[n : n + 1], (LANES, LANES)).T
        row_rate[here] = jnp.broadcast_to(rate[n : n + 1], (LANES, LANES)).T
    await_bytes(expert_total, sum_recv.at[3])
    totals = {(0, 0, 0): square_part}
    for n, key in enumerate(experts):
        totals[key] = expert_total[n]
    chips = [[totals[(dy, dx, 0)] + totals[(dy, dx, 1)] for dx in range(4)] for dy in range(2)]
    squared_total = full_sum(ring_sum(chips[0]) + ring_sum(chips[1]))
    clip = 1.0 / jnp.maximum(1.0, jnp.sqrt(squared_total / (matrices * entries)))
    clip_square = clip * clip
    one = clip_square[:1, :1]
    fresh_cols = col_total * one + model_width * EPS
    cols_now = DECAY * col_state[...] + (1.0 - DECAY) * (fresh_cols / model_width)
    col_scale[...] = 1.0 / cols_now

    def weigh(i, total):
        here = pl.ds(pl.multiple_of(i * 64, 64), 64)
        line = None
        for lane in lanes:
            block = squares[here, lane] * col_scale[:, lane]
            line = block if line is None else line + block
        line = line / (row_base[here] + row_rate[here] * one)
        return total + jnp.sum(line.reshape(8, 8, LANES), axis=0)

    update_part[...] = lax.fori_loop(0, rows // 64, weigh, jnp.zeros((8, LANES), F32))
    for dr, dc in peers:
        n = dr * 4 + dc - 1
        remote(update_part, group_update.at[n], send_sem.at[9], sum_recv.at[4], group[(dr, (4 - dc) % 4)]).start()
    new_rows[...] = base + rate * one
    new_cols[...] = cols_now
    average = DECAY * (old_total / model_width) + (1.0 - DECAY) * (group_squares * clip_square / entries + EPS)

    @pl.loop(0, rows // 64)
    def _(i):
        here = pl.ds(pl.multiple_of(i * 64, 64), 64)
        row_scale[here] = 1.0 / jnp.sqrt(row_base[here] + row_rate[here] * one)

    col_root = jnp.sqrt(col_scale[...])
    scale = clip * jnp.sqrt(average) * jnp.sqrt(weight_total / entries)
    await_bytes(y_send, send_sem.at[0])
    await_bytes(xg.at[pl.ds(0, 4 * tokens)], send_sem.at[1])
    await_bytes(xg.at[pl.ds(0, 2 * tokens)], send_sem.at[2])
    cross_x.wait_send()
    await_bytes(yg.at[pl.ds(0, 4 * tokens)], send_sem.at[4])
    await_bytes(group_small, send_sem.at[5])
    await_bytes(ring_rows, send_sem.at[6])
    pair_copy.wait_send()
    await_bytes(expert_total, send_sem.at[8])
    await_bytes(group_update, send_sem.at[9])
    await_bytes(group_update, sum_recv.at[4])
    parts = {(0, 0): update_part[...]}
    for dr, dc in peers:
        parts[(dr, dc)] = group_update[dr * 4 + dc - 1]
    update_total = full_sum(group_sum(parts)) * clip_square * average
    factor = scale / jnp.maximum(1.0, jnp.sqrt(update_total / entries))
    col_scale[...] = col_root * factor[:1, :1]


def scale_kernel(grad, row_scale, col_scale, rows_in, cols_in, out, rows_out, cols_out, scaled, sem):
    rows, cols = grad.shape
    height = 64
    rows_copy = pltpu.make_async_copy(rows_in, rows_out, sem.at[1])
    cols_copy = pltpu.make_async_copy(cols_in, cols_out, sem.at[2])
    rows_copy.start()
    cols_copy.start()

    @pl.loop(0, rows // height)
    def _(step):
        for i in range(height // 8):
            here = pl.ds(pl.multiple_of(step * height + i * 8, 8), 8)
            scale = row_scale[here]
            for n in range(cols // LANES):
                lane = slice(n * LANES, (n + 1) * LANES)
                scaled[here, lane] = grad[here, lane] * scale * col_scale[:, lane]
        block = pl.ds(pl.multiple_of(step * height, height), height)
        pltpu.make_async_copy(scaled.at[block], out.at[block], sem.at[0]).start()

    rows_copy.wait()
    cols_copy.wait()
    pltpu.make_async_copy(scaled, out, sem.at[0]).wait()


def body(weights, inputs, cotangents, row_state, col_state):
    _, rows, cols = weights.shape
    tokens = inputs.shape[1]
    lines = rows // LANES
    vmem = pl.BlockSpec(memory_space=pltpu.VMEM)
    anywhere = pl.BlockSpec(memory_space=pl.ANY)
    shapes = [
        pltpu.VMEM((rows, cols), F32),
        pltpu.VMEM((rows, LANES), F32),
        pltpu.VMEM((1, cols), F32),
        pltpu.VMEM((lines, LANES), F32),
        pltpu.VMEM((1, cols), F32),
    ]
    sub = rows // 2 // SUBS
    dma = pltpu.SemaphoreType.DMA
    grad, row_scale, col_scale, new_rows, new_cols = pl.pallas_call(
        gather_kernel,
        name="gather_gradient",
        out_shape=shapes,
        in_specs=[anywhere] * 5,
        out_specs=[vmem] * 5,
        scratch_shapes=[
            pltpu.VMEM((8 * tokens, rows), BF16),
            pltpu.VMEM((8 * tokens, cols), BF16),
            pltpu.VMEM((rows, 6 * tokens), BF16),
            pltpu.VMEM((rows, 2 * tokens), BF16),
            pltpu.VMEM((tokens, rows), BF16),
            pltpu.VMEM((3, tokens, cols), BF16),
            pltpu.VMEM((2, 256, cols), BF16),
            pltpu.VMEM((lines, LANES), F32),
            pltpu.VMEM((1, cols), F32),
            pltpu.VMEM((8, cols), F32),
            pltpu.VMEM((rows, cols), F32),
            pltpu.VMEM((rows, LANES), F32),
            pltpu.VMEM((rows, LANES), F32),
            pltpu.VMEM((rows, LANES), F32),
            pltpu.VMEM((8, cols), F32),
            pltpu.VMEM((lines, LANES), F32),
            pltpu.VMEM((1, cols), F32),
            pltpu.VMEM((24, LANES), F32),
            pltpu.VMEM((3, lines, LANES), F32),
            pltpu.VMEM((1, cols), F32),
            pltpu.VMEM((7, 24, LANES), F32),
            pltpu.VMEM((8, LANES), F32),
            pltpu.VMEM((15, 8, LANES), F32),
            pltpu.VMEM((8, LANES), F32),
            pltpu.VMEM((7, 8, LANES), F32),
            dma((8,)), dma((2,)), dma((10,)), dma((3,)), dma((4,)), dma((SUBS,)), dma((8,)), dma((5,)),
        ],
        compiler_params=pltpu.CompilerParams(collective_id=0, has_side_effects=True, vmem_limit_bytes=40 * 2**20),
        cost_estimate=pl.CostEstimate(flops=16 * tokens * rows * cols, bytes_accessed=2**23, transcendentals=0),
    )(weights, inputs, cotangents, row_state.reshape(lines, LANES), col_state)
    out, rows_out, cols_out = pl.pallas_call(
        scale_kernel,
        name="scale_update",
        out_shape=[
            jax.ShapeDtypeStruct((rows, cols), F32),
            jax.ShapeDtypeStruct((lines, LANES), F32),
            jax.ShapeDtypeStruct((1, cols), F32),
        ],
        in_specs=[vmem] * 5,
        out_specs=[anywhere] * 3,
        scratch_shapes=[pltpu.VMEM((rows, cols), F32), dma((3,))],
        compiler_params=pltpu.CompilerParams(vmem_limit_bytes=20 * 2**20),
    )(grad, row_scale, col_scale, new_rows, new_cols)
    return out.reshape(1, rows, cols), rows_out.reshape(1, rows), cols_out


def solution(mesh):
    split = Mesh(
        mesh.devices.reshape(2, 4, 2, mesh.shape["row"], mesh.shape["col"]),
        (*EXPERT, "row", "col"),
    )
    return jax.shard_map(
        body,
        mesh=split,
        in_specs=(
            P(EXPERT, "row", "col"),
            P(EXPERT, ("row", "col"), None),
            P(EXPERT, ("row", "col"), None),
            P(EXPERT, "row"),
            P(EXPERT, "col"),
        ),
        out_specs=(P(EXPERT, "row", "col"), P(EXPERT, "row"), P(EXPERT, "col")),
        check_vma=False,
    )
```

```python
import itertools

import jax
import jax.numpy as jnp
from jax import lax
from jax.experimental import pallas as pl
from jax.experimental.pallas import tpu as pltpu
from jax.sharding import Mesh
from jax.sharding import PartitionSpec as P

STEP = 10
EPS = 1e-30
DECAY = 1.0 - STEP ** (-0.8)
EXPERT = ("ylo", "x", "core")
MESH = pl.DeviceIdType.MESH
F32 = jnp.float32
BF16 = jnp.bfloat16
SUBS = 8
LANES = 128
FORWARD_SEM = (0, 0, 1, 1, 2, 2, 3, 4)
LAST_STEPS = ((0, 3), (3, 6), (6, 7))
PLACE = (0, 1, 3, 2)


def neighbours():
    lengths = (2, 4, 2, 2, 4)
    axes = (*EXPERT, "row", "col")
    here = [lax.axis_index(axis) for axis in axes]
    places = [[lax.rem(at + step, length) for step in range(length)] for at, length in zip(here, lengths)]
    steps = [s for s in itertools.product(*map(range, lengths)) if any(s)]
    hops = (1, (0, 1, 2, 1), 0, 2, (0, 1, 2, 1))
    far = lambda s: sum(h[k] if isinstance(h, tuple) else h * k for h, k in zip(hops, s))
    steps.sort(key=far, reverse=True)
    return {s: {axis: places[n][s[n]] for n, axis in enumerate(axes) if s[n]} for s in steps}


def back(step):
    return tuple((length - k) % length for k, length in zip(step, (2, 4, 2, 2, 4)))


def ring_sum(parts):
    return (parts[0] + parts[2]) + (parts[1] + parts[3])


def group_sum(parts):
    return ring_sum([parts[(0, c)] for c in range(4)]) + ring_sum([parts[(1, c)] for c in range(4)])


def full_sum(vector):
    return jnp.broadcast_to(jnp.sum(vector, keepdims=True), vector.shape)


def gather_kernel(
    weights, inputs, cotangents, row_state_in, col_state_in,
    grad, row_scale, col_scale, new_rows, new_cols,
    xg, yg, xt, xt_last, x_send, y_send, w_buf, row_state, col_state,
    w_acc, squares, row_base, row_rate, row_part, col_part, row_vec, col_vec, early, sent,
    ring_rows, pair_cols, group_early, gathered,
    local_sem, w_sem, send_sem, yz_recv, xz_recv, fw_recv, cross_recv, sum_recv,
):
    tokens = inputs.shape[1]
    rows, cols = grad.shape
    half, pair = rows // 2, 2 * tokens
    sub = half // SUBS
    row, col = lax.axis_index("row"), lax.axis_index("col")
    everyone = neighbours()
    group = {key[3:]: device for key, device in everyone.items() if not any(key[:3])}
    peers = list(group)
    greeted = [device for key, device in everyone.items() if not any(key[:3]) or not any(key[3:])]
    up, down, across = group[(0, 1)], group[(0, 3)], group[(0, 2)]
    partner = group[(1, 0)]

    def remote(src, dst, send, recv, device):
        return pltpu.make_async_remote_copy(
            src_ref=src, dst_ref=dst, send_sem=send, recv_sem=recv, device_id=device, device_id_type=MESH
        )

    def tokens_of(buffer, j, s, width=None):
        start = PLACE[j] * pair + s * tokens
        if width is None:
            return buffer.at[pl.ds(start, tokens)]
        return buffer.at[pl.ds(start, tokens), width]

    def row_cols(r):
        return pl.ds(pl.multiple_of(r * rows, rows), rows)

    def col_cols(c):
        return pl.ds(pl.multiple_of(c * cols, cols), cols)

    y_dest = (1, 3, 2)
    local = []
    for n, dc in enumerate(y_dest):
        local.append((cotangents.at[0, :, col_cols(lax.rem(col + dc, 4))], y_send.at[n]))
    local.append((inputs.at[0, :, row_cols(1 - row)], x_send))
    local.append((inputs.at[0, :, row_cols(row)], tokens_of(xg, 0, 0)))
    local.append((cotangents.at[0, :, col_cols(col)], tokens_of(yg, 0, 0)))
    loads = [pltpu.make_async_copy(s, d, local_sem.at[n]) for n, (s, d) in enumerate(local)]
    loads.append(pltpu.make_async_copy(row_state_in, row_state, local_sem.at[6]))
    loads.append(pltpu.make_async_copy(col_state_in, col_state, local_sem.at[7]))
    for n in (0, 1, 3, 4, 5, 2, 6, 7):
        loads[n].start()
    w_rows = w_buf.shape[1]
    w_steps = rows // w_rows

    def w_load(step, slot):
        start = pl.multiple_of(step * w_rows, w_rows)
        return pltpu.make_async_copy(weights.at[0, pl.ds(start, w_rows)], w_buf.at[slot], w_sem.at[slot])

    w_load(0, 0).start()

    barrier = pltpu.get_barrier_semaphore()
    for device in greeted:
        pl.semaphore_signal(barrier, inc=1, device_id=device, device_id_type=MESH)
    pl.semaphore_wait(barrier, len(greeted))

    y_copies = []
    for n, (dc, device) in enumerate(zip(y_dest, (up, down, across))):
        y_copies.append(
            remote(y_send.at[n], tokens_of(yg, (4 - dc) % 4, 0), send_sem.at[0], yz_recv.at[n], device)
        )
    lower, upper = pl.ds(0, half), pl.ds(half, half)

    def x_copy(s, direction, part):
        device, j = ((up, 3), (down, 1))[direction]
        width = (lower, upper)[direction ^ part]
        recv = xz_recv.at[s * 2 + part]
        return remote(tokens_of(xg, 0, s, width), tokens_of(xg, j, s, width), send_sem.at[0], recv, device)

    def forward(s, direction, step):
        device, j = ((up, 3), (down, 1))[direction]
        width = pl.ds(direction * half + step * sub, sub)
        return remote(
            tokens_of(xg, j, s, width), tokens_of(xg, 2, s, width), send_sem.at[0], fw_recv.at[FORWARD_SEM[step]], device
        )

    def await_bytes(like, sem):
        pltpu.make_async_copy(like, like, sem).wait()

    cross_x = remote(x_send, tokens_of(xg, 0, 1), send_sem.at[0], cross_recv.at[2], partner)
    cross_y = {
        j: remote(tokens_of(yg, j, 0), tokens_of(yg, j, 1), send_sem.at[0], cross_recv.at[j], partner) for j in (0, 1, 3)
    }
    n_width = 2 * LANES
    n_steps = cols // n_width
    cross_last = []
    for n, (first, end) in enumerate(LAST_STEPS):
        width = pl.ds(first * n_width, (end - first) * n_width)
        recv = cross_recv.at[4 + n]
        cross_last.append(remote(tokens_of(yg, 2, 0, width), tokens_of(yg, 2, 1, width), send_sem.at[0], recv, partner))

    loads[0].wait()
    y_copies[0].start()
    loads[1].wait()
    y_copies[1].start()
    loads[3].wait()
    cross_x.start()
    loads[4].wait()
    for part in range(2):
        for direction in range(2):
            x_copy(0, direction, part).start()
    loads[5].wait()
    cross_y[0].start()
    loads[2].wait()
    y_copies[2].start()

    w_acc[...] = jnp.zeros_like(w_acc)

    @pl.loop(0, w_steps)
    def _(step):
        slot = lax.rem(step, 2)

        @pl.when(step + 1 < w_steps)
        def _():
            w_load(step + 1, 1 - slot).start()

        w_load(step, slot).wait()

        def add(i, total):
            block = w_buf[slot, pl.ds(pl.multiple_of(i * 16, 16), 16), :].astype(F32)
            block = block * block
            return total + (block[:8] + block[8:])

        w_acc[...] = lax.fori_loop(0, w_rows // 16, add, w_acc[...])

    weight_part = w_acc[:, :LANES]
    for n in range(1, cols // LANES):
        weight_part += w_acc[:, n * LANES : (n + 1) * LANES]
    early[0:1] = jnp.sum(weight_part, axis=0, keepdims=True)
    loads[6].wait()
    loads[7].wait()
    old_rows = row_state[...]
    early[1:2] = jnp.sum(old_rows, axis=0, keepdims=True)
    for dr, dc in peers:
        n = dr * 4 + dc - 1
        remote(early, group_early.at[n], send_sem.at[1], sum_recv.at[0], group[(dr, (4 - dc) % 4)]).start()

    def turn(first, count, start, width):
        @pl.loop(0, width // LANES)
        def _(i):
            at = pl.multiple_of(start + i * LANES, LANES)
            block = xg[first * pair : (first + count) * pair, pl.ds(at, LANES)]
            xt[pl.ds(at, LANES), first * pair : (first + count) * pair] = block.T

    def multiply(place, halves, fresh=False):
        depth = slice(place * pair, (place + 1) * pair)

        for n in range(n_steps):
            at = slice(n * n_width, (n + 1) * n_width)
            for m in halves:
                here = slice(m * half, (m + 1) * half)
                part = jnp.dot(xt[here, depth], yg[depth, at], preferred_element_type=F32)
                if not fresh:
                    part += grad[here, at]
                grad[here, at] = part

    y_copies[0].wait_recv()
    y_copies[1].wait_recv()
    cross_y[3].start()
    cross_y[1].start()
    cross_x.wait_recv()
    for part in range(2):
        for direction in range(2):
            x_copy(1, direction, part).start()
    turn(0, 1, 0, rows)
    cross_y[0].wait_recv()
    multiply(0, (0, 1), fresh=True)
    y_copies[2].wait_recv()
    for copy in cross_last:
        copy.start()

    await_bytes(x_send, xz_recv.at[0])
    await_bytes(x_send, xz_recv.at[2])
    for step in range(SUBS):
        for s in range(2):
            for direction in range(2):
                forward(s, direction, step).start()
    turn(2, 1, 0, half)
    turn(1, 1, half, half)
    cross_y[3].wait_recv()
    multiply(2, (0,))
    cross_y[1].wait_recv()
    multiply(1, (1,))
    await_bytes(x_send, xz_recv.at[1])
    await_bytes(x_send, xz_recv.at[3])
    turn(2, 1, half, half)
    turn(1, 1, 0, half)
    multiply(2, (1,))
    multiply(1, (0,))
    col_part[...] = jnp.zeros_like(col_part)
    last = slice(PLACE[2] * pair, (PLACE[2] + 1) * pair)
    lanes = [slice(n * LANES, (n + 1) * LANES) for n in range(cols // LANES)]

    def await_forward(*steps):
        await_bytes(x_send.at[:, pl.ds(0, 4 * sub * len(steps))], fw_recv.at[FORWARD_SEM[steps[0]]])
        for step in steps:
            for direction in range(2):
                at = direction * half + step * sub
                to = (2 * step + direction) * sub
                xt_last[to : to + sub, :] = xg[last, at : at + sub].T

    def finish(first, end, steps, row_sums=False):
        for n in range(*steps):
            at = slice(n * n_width, (n + 1) * n_width)
            part = jnp.dot(xt_last[first * 2 * sub : end * 2 * sub], yg[last, at], preferred_element_type=F32)
            total = col_part[:, at]
            for step in range(first, end):
                for direction in range(2):
                    here = slice(direction * half + step * sub, direction * half + (step + 1) * sub)
                    begin = (2 * (step - first) + direction) * sub
                    block = part[begin : begin + sub] + grad[here, at]
                    grad[here, at] = block
                    block = block * block
                    total += jnp.sum(block.reshape(sub // 8, 8, n_width), axis=0)
                    if row_sums:
                        block = block[:, :LANES] + block[:, LANES:]
                        row_part[here] = block if n == 0 else row_part[here] + block
            col_part[:, at] = total

    def sum_rows(first, end):
        for direction in range(2):

            @pl.loop(first * sub // 32, end * sub // 32)
            def _(i):
                for k in range(4):
                    here = pl.ds(pl.multiple_of(direction * half + i * 32 + k * 8, 8), 8)
                    sums = [None, None]
                    for n, lane in enumerate(lanes):
                        block = grad[here, lane]
                        block = block * block
                        sums[n % 2] = block if sums[n % 2] is None else sums[n % 2] + block
                    row_part[here] = sums[0] + sums[1]

    def turn_sums():
        for n in range(rows // LANES):
            turned = row_part[n * LANES : (n + 1) * LANES].T
            row_vec[n : n + 1] = jnp.sum(turned, axis=0, keepdims=True)

    def square():
        @pl.loop(0, rows // 32)
        def _(i):
            here = pl.ds(pl.multiple_of(i * 32, 32), 32)
            block = grad[here, :]
            squares[here, :] = block * block

    await_forward(0, 1)
    cross_last[0].wait_recv()
    finish(0, 2, LAST_STEPS[0])
    await_forward(2, 3)
    finish(2, 4, LAST_STEPS[0])
    cross_last[1].wait_recv()
    finish(0, 4, LAST_STEPS[1])
    await_forward(4, 5)
    finish(4, 6, (0, LAST_STEPS[1][1]))
    cross_last[2].wait_recv()
    finish(0, 6, LAST_STEPS[2])
    await_forward(6)
    finish(6, 7, (0, n_steps), row_sums=True)
    await_forward(7)
    finish(7, 8, (0, n_steps), row_sums=True)

    square_part = col_part[:, :LANES]
    for lane in lanes[1:]:
        square_part += col_part[:, lane]
    square_part = jnp.sum(square_part, axis=0, keepdims=True)
    sent[0] = square_part
    for n, key in enumerate(everyone):
        remote(sent.at[0], gathered.at[n], send_sem.at[2], sum_recv.at[3], everyone[back(key)]).start()
    sum_rows(0, 6)
    turn_sums()
    for dc in (1, 2, 3):
        remote(row_vec, ring_rows.at[dc - 1], send_sem.at[4], sum_recv.at[1], group[(0, (4 - dc) % 4)]).start()
    col_vec[...] = jnp.sum(col_part[...], axis=0, keepdims=True)
    pair_copy = remote(col_vec, pair_cols, send_sem.at[3], sum_recv.at[2], partner)
    pair_copy.start()
    square()
    model_width, hidden_width = 2 * rows, 4 * cols
    entries = model_width * hidden_width
    matrices = (1 + len(everyone)) // (1 + len(peers))
    await_bytes(group_early, sum_recv.at[0])
    early_parts = {(0, 0): early[...]}
    for dr, dc in peers:
        early_parts[(dr, dc)] = group_early[dr * 4 + dc - 1]
    weight_total = full_sum(group_sum(early_parts)[0:1])
    old_total = full_sum((early_parts[(0, 0)] + early_parts[(1, 0)])[1:2])
    await_bytes(ring_rows, sum_recv.at[1])
    pair_copy.wait_recv()
    row_total = ring_sum([row_vec[...], ring_rows[0], ring_rows[1], ring_rows[2]])
    col_total = col_vec[...] + pair_cols[...]
    base = DECAY * row_state[...] + (1.0 - DECAY) * EPS
    rate = (1.0 - DECAY) * (row_total / hidden_width)
    for n in range(rows // LANES):
        here = slice(n * LANES, (n + 1) * LANES)
        row_base[here] = jnp.broadcast_to(base[n : n + 1], (LANES, LANES)).T
        row_rate[here] = jnp.broadcast_to(rate[n : n + 1], (LANES, LANES)).T
    await_bytes(gathered.at[pl.ds(0, len(everyone))], sum_recv.at[3])
    parts = {(0, 0, 0, 0, 0): square_part}
    for n, key in enumerate(everyone):
        parts[key] = gathered[n]
    groups = {}
    for expert in itertools.product(range(2), range(4), range(2)):
        groups[expert] = group_sum({key[3:]: part for key, part in parts.items() if key[:3] == expert})
    chips = [[groups[(dy, dx, 0)] + groups[(dy, dx, 1)] for dx in range(4)] for dy in range(2)]
    squared_total = full_sum(ring_sum(chips[0]) + ring_sum(chips[1]))
    group_squares = full_sum(groups[(0, 0, 0)])
    clip = 1.0 / jnp.maximum(1.0, jnp.sqrt(squared_total / (matrices * entries)))
    clip_square = clip * clip
    one = clip_square[:, :1]
    fresh_cols = col_total * one + model_width * EPS
    cols_now = DECAY * col_state[...] + (1.0 - DECAY) * (fresh_cols / model_width)
    col_scale[...] = 1.0 / cols_now

    def weigh(i, total):
        here = pl.ds(pl.multiple_of(i * 64, 64), 64)
        line = None
        for lane in lanes:
            block = squares[here, lane] * col_scale[:, lane]
            line = block if line is None else line + block
        line = line / (row_base[here] + row_rate[here] * one)
        return total + jnp.sum(line.reshape(8, 8, LANES), axis=0)

    update_part = lax.fori_loop(0, rows // 64, weigh, jnp.zeros((8, LANES), F32), unroll=2)
    update_part = jnp.sum(update_part, axis=0, keepdims=True)
    sent[1] = update_part
    first = len(everyone)
    for dr, dc in peers:
        n = first + dr * 4 + dc - 1
        remote(sent.at[1], gathered.at[n], send_sem.at[2], sum_recv.at[5], group[(dr, (4 - dc) % 4)]).start()
    new_rows[...] = base + rate * one
    new_cols[...] = cols_now
    average = DECAY * (old_total / model_width) + (1.0 - DECAY) * (group_squares * clip_square / entries + EPS)

    @pl.loop(0, rows // 64)
    def _(i):
        here = pl.ds(pl.multiple_of(i * 64, 64), 64)
        row_scale[here] = 1.0 / jnp.sqrt(row_base[here] + row_rate[here] * one)

    col_root = jnp.sqrt(col_scale[...])
    scale = clip * jnp.sqrt(average) * jnp.sqrt(weight_total / entries)
    sent_bytes = (5 * tokens * rows + 2 * tokens * rows + 7 * tokens * cols) * 2
    await_bytes(squares.at[pl.ds(0, sent_bytes // (4 * cols))], send_sem.at[0])
    await_bytes(group_early, send_sem.at[1])
    await_bytes(ring_rows, send_sem.at[4])
    pair_copy.wait_send()
    await_bytes(gathered, send_sem.at[2])
    await_bytes(gathered.at[pl.ds(first, len(peers))], sum_recv.at[5])
    parts = {(0, 0): update_part}
    for dr, dc in peers:
        parts[(dr, dc)] = gathered[first + dr * 4 + dc - 1]
    update_total = full_sum(group_sum(parts)) * clip_square * average
    factor = scale / jnp.maximum(1.0, jnp.sqrt(update_total / entries))
    col_scale[...] = col_root * factor[:, :1]


def scale_kernel(grad, row_scale, col_scale, rows_in, cols_in, out, rows_out, cols_out, scaled, sem):
    rows, cols = grad.shape
    height = 64
    rows_copy = pltpu.make_async_copy(rows_in, rows_out, sem.at[1])
    cols_copy = pltpu.make_async_copy(cols_in, cols_out, sem.at[2])
    rows_copy.start()
    cols_copy.start()

    @pl.loop(0, rows // height)
    def _(step):
        for i in range(height // 8):
            here = pl.ds(pl.multiple_of(step * height + i * 8, 8), 8)
            scale = row_scale[here]
            for n in range(cols // LANES):
                lane = slice(n * LANES, (n + 1) * LANES)
                scaled[here, lane] = grad[here, lane] * scale * col_scale[:, lane]
        block = pl.ds(pl.multiple_of(step * height, height), height)
        pltpu.make_async_copy(scaled.at[block], out.at[block], sem.at[0]).start()

    rows_copy.wait()
    cols_copy.wait()
    pltpu.make_async_copy(scaled, out, sem.at[0]).wait()


def body(weights, inputs, cotangents, row_state, col_state):
    _, rows, cols = weights.shape
    tokens = inputs.shape[1]
    lines = rows // LANES
    vmem = pl.BlockSpec(memory_space=pltpu.VMEM)
    anywhere = pl.BlockSpec(memory_space=pl.ANY)
    shapes = [
        pltpu.VMEM((rows, cols), F32),
        pltpu.VMEM((rows, LANES), F32),
        pltpu.VMEM((1, cols), F32),
        pltpu.VMEM((lines, LANES), F32),
        pltpu.VMEM((1, cols), F32),
    ]
    sub = rows // 2 // SUBS
    dma = pltpu.SemaphoreType.DMA
    grad, row_scale, col_scale, new_rows, new_cols = pl.pallas_call(
        gather_kernel,
        name="gather_gradient",
        out_shape=shapes,
        in_specs=[anywhere] * 5,
        out_specs=[vmem] * 5,
        scratch_shapes=[
            pltpu.VMEM((8 * tokens, rows), BF16),
            pltpu.VMEM((8 * tokens, cols), BF16),
            pltpu.VMEM((rows, 6 * tokens), BF16),
            pltpu.VMEM((rows, 2 * tokens), BF16),
            pltpu.VMEM((tokens, rows), BF16),
            pltpu.VMEM((3, tokens, cols), BF16),
            pltpu.VMEM((2, 256, cols), BF16),
            pltpu.VMEM((lines, LANES), F32),
            pltpu.VMEM((1, cols), F32),
            pltpu.VMEM((8, cols), F32),
            pltpu.VMEM((rows, cols), F32),
            pltpu.VMEM((rows, LANES), F32),
            pltpu.VMEM((rows, LANES), F32),
            pltpu.VMEM((rows, LANES), F32),
            pltpu.VMEM((8, cols), F32),
            pltpu.VMEM((lines, LANES), F32),
            pltpu.VMEM((1, cols), F32),
            pltpu.VMEM((2, LANES), F32),
            pltpu.VMEM((2, 1, LANES), F32),
            pltpu.VMEM((3, lines, LANES), F32),
            pltpu.VMEM((1, cols), F32),
            pltpu.VMEM((7, 2, LANES), F32),
            pltpu.VMEM((134, 1, LANES), F32),
            dma((8,)), dma((2,)), dma((5,)), dma((3,)), dma((4,)), dma((5,)), dma((7,)), dma((6,)),
        ],
        compiler_params=pltpu.CompilerParams(collective_id=0, has_side_effects=True, vmem_limit_bytes=40 * 2**20),
        cost_estimate=pl.CostEstimate(flops=16 * tokens * rows * cols, bytes_accessed=2**23, transcendentals=0),
    )(weights, inputs, cotangents, row_state.reshape(lines, LANES), col_state)
    out, rows_out, cols_out = pl.pallas_call(
        scale_kernel,
        name="scale_update",
        out_shape=[
            jax.ShapeDtypeStruct((rows, cols), F32),
            jax.ShapeDtypeStruct((lines, LANES), F32),
            jax.ShapeDtypeStruct((1, cols), F32),
        ],
        in_specs=[vmem] * 5,
        out_specs=[anywhere] * 3,
        scratch_shapes=[pltpu.VMEM((rows, cols), F32), dma((3,))],
        compiler_params=pltpu.CompilerParams(vmem_limit_bytes=20 * 2**20),
    )(grad, row_scale, col_scale, new_rows, new_cols)
    return out.reshape(1, rows, cols), rows_out.reshape(1, rows), cols_out


def solution(mesh):
    split = Mesh(
        mesh.devices.reshape(2, 4, 2, mesh.shape["row"], mesh.shape["col"]),
        (*EXPERT, "row", "col"),
    )
    return jax.shard_map(
        body,
        mesh=split,
        in_specs=(
            P(EXPERT, "row", "col"),
            P(EXPERT, ("row", "col"), None),
            P(EXPERT, ("row", "col"), None),
            P(EXPERT, "row"),
            P(EXPERT, "col"),
        ),
        out_specs=(P(EXPERT, "row", "col"), P(EXPERT, "row"), P(EXPERT, "col")),
        check_vma=False,
    )
```

```python
import itertools

import jax
import jax.numpy as jnp
from jax import lax
from jax.experimental import pallas as pl
from jax.experimental.pallas import tpu as pltpu
from jax.sharding import Mesh
from jax.sharding import PartitionSpec as P

STEP = 10
EPS = 1e-30
DECAY = 1.0 - STEP ** (-0.8)
EXPERT = ("ylo", "x", "core")
MESH = pl.DeviceIdType.MESH
F32 = jnp.float32
BF16 = jnp.bfloat16
SUBS = 8
LANES = 128
FORWARD_SEM = (0, 0, 1, 1, 2, 3, 4, 5)
LAST_STEPS = ((0, 3), (3, 6), (6, 7))
PLACE = (0, 1, 3, 2)


def neighbours():
    lengths = (2, 4, 2, 2, 4)
    axes = (*EXPERT, "row", "col")
    here = [lax.axis_index(axis) for axis in axes]
    places = [[lax.rem(at + step, length) for step in range(length)] for at, length in zip(here, lengths)]
    steps = [s for s in itertools.product(*map(range, lengths)) if any(s)]
    hops = (1, (0, 1, 2, 1), 0, 2, (0, 1, 2, 1))
    far = lambda s: sum(h[k] if isinstance(h, tuple) else h * k for h, k in zip(hops, s))
    steps.sort(key=far, reverse=True)
    return {s: {axis: places[n][s[n]] for n, axis in enumerate(axes) if s[n]} for s in steps}


def back(step):
    return tuple((length - k) % length for k, length in zip(step, (2, 4, 2, 2, 4)))


def ring_sum(parts):
    return (parts[0] + parts[2]) + (parts[1] + parts[3])


def group_sum(parts):
    return ring_sum([parts[(0, c)] for c in range(4)]) + ring_sum([parts[(1, c)] for c in range(4)])


def full_sum(vector):
    return jnp.broadcast_to(jnp.sum(vector, keepdims=True), vector.shape)


def gather_kernel(
    weights, inputs, cotangents, row_state_in, col_state_in,
    grad, row_scale, col_scale, new_rows, new_cols,
    xg, yg, xt, xt_last, x_send, y_send, w_buf, row_state, col_state,
    w_acc, squares, row_base, row_rate, row_part, col_part, row_vec, col_vec, early, sent,
    ring_rows, pair_cols, group_early, gathered,
    local_sem, w_sem, send_sem, yz_recv, xz_recv, fw_recv, cross_recv, sum_recv,
):
    tokens = inputs.shape[1]
    rows, cols = grad.shape
    half, pair = rows // 2, 2 * tokens
    sub = half // SUBS
    row, col = lax.axis_index("row"), lax.axis_index("col")
    everyone = neighbours()
    group = {key[3:]: device for key, device in everyone.items() if not any(key[:3])}
    peers = list(group)
    greeted = [device for key, device in everyone.items() if not any(key[:3]) or not any(key[3:])]
    up, down, across = group[(0, 1)], group[(0, 3)], group[(0, 2)]
    partner = group[(1, 0)]

    def remote(src, dst, send, recv, device):
        return pltpu.make_async_remote_copy(
            src_ref=src, dst_ref=dst, send_sem=send, recv_sem=recv, device_id=device, device_id_type=MESH
        )

    def tokens_of(buffer, j, s, width=None):
        start = PLACE[j] * pair + s * tokens
        if width is None:
            return buffer.at[pl.ds(start, tokens)]
        return buffer.at[pl.ds(start, tokens), width]

    def row_cols(r):
        return pl.ds(pl.multiple_of(r * rows, rows), rows)

    def col_cols(c):
        return pl.ds(pl.multiple_of(c * cols, cols), cols)

    y_dest = (1, 3, 2)
    local = []
    for n, dc in enumerate(y_dest):
        local.append((cotangents.at[0, :, col_cols(lax.rem(col + dc, 4))], y_send.at[n]))
    local.append((inputs.at[0, :, row_cols(1 - row)], x_send))
    local.append((inputs.at[0, :, row_cols(row)], tokens_of(xg, 0, 0)))
    local.append((cotangents.at[0, :, col_cols(col)], tokens_of(yg, 0, 0)))
    loads = [pltpu.make_async_copy(s, d, local_sem.at[n]) for n, (s, d) in enumerate(local)]
    loads.append(pltpu.make_async_copy(row_state_in, row_state, local_sem.at[6]))
    loads.append(pltpu.make_async_copy(col_state_in, col_state, local_sem.at[7]))
    for n in (0, 1, 3, 4, 5, 2, 6, 7):
        loads[n].start()
    w_rows = w_buf.shape[1]
    w_steps = rows // w_rows

    def w_load(step, slot):
        start = pl.multiple_of(step * w_rows, w_rows)
        return pltpu.make_async_copy(weights.at[0, pl.ds(start, w_rows)], w_buf.at[slot], w_sem.at[slot])

    w_load(0, 0).start()

    barrier = pltpu.get_barrier_semaphore()
    for device in greeted:
        pl.semaphore_signal(barrier, inc=1, device_id=device, device_id_type=MESH)
    pl.semaphore_wait(barrier, len(greeted))

    y_copies = []
    for n, (dc, device) in enumerate(zip(y_dest, (up, down, across))):
        y_copies.append(
            remote(y_send.at[n], tokens_of(yg, (4 - dc) % 4, 0), send_sem.at[0], yz_recv.at[n // 2], device)
        )
    lower, upper = pl.ds(0, half), pl.ds(half, half)

    def x_copy(s, direction, part):
        device, j = ((up, 3), (down, 1))[direction]
        width = (lower, upper)[direction ^ part]
        recv = xz_recv.at[part]
        return remote(tokens_of(xg, 0, s, width), tokens_of(xg, j, s, width), send_sem.at[0], recv, device)

    def forward(s, direction, step):
        device, j = ((up, 3), (down, 1))[direction]
        width = pl.ds(direction * half + step * sub, sub)
        return remote(
            tokens_of(xg, j, s, width), tokens_of(xg, 2, s, width), send_sem.at[0], fw_recv.at[FORWARD_SEM[step]], device
        )

    def await_bytes(like, sem):
        pltpu.make_async_copy(like, like, sem).wait()

    cross_x = remote(x_send, tokens_of(xg, 0, 1), send_sem.at[0], cross_recv.at[2], partner)
    cross_y = {
        j: remote(tokens_of(yg, j, 0), tokens_of(yg, j, 1), send_sem.at[0], cross_recv.at[j], partner) for j in (0, 1, 3)
    }
    n_width = 2 * LANES
    n_steps = cols // n_width
    cross_last = []
    for n, (first, end) in enumerate(LAST_STEPS):
        width = pl.ds(first * n_width, (end - first) * n_width)
        recv = cross_recv.at[4 + n]
        cross_last.append(remote(tokens_of(yg, 2, 0, width), tokens_of(yg, 2, 1, width), send_sem.at[0], recv, partner))

    loads[0].wait()
    y_copies[0].start()
    loads[1].wait()
    y_copies[1].start()
    loads[3].wait()
    cross_x.start()
    loads[4].wait()
    for part in range(2):
        for direction in range(2):
            x_copy(0, direction, part).start()
    loads[5].wait()
    cross_y[0].start()
    loads[2].wait()
    y_copies[2].start()

    w_acc[...] = jnp.zeros_like(w_acc)

    @pl.loop(0, w_steps)
    def _(step):
        slot = lax.rem(step, 2)

        @pl.when(step + 1 < w_steps)
        def _():
            w_load(step + 1, 1 - slot).start()

        w_load(step, slot).wait()

        def add(i, total):
            block = w_buf[slot, pl.ds(pl.multiple_of(i * 16, 16), 16), :].astype(F32)
            block = block * block
            return total + (block[:8] + block[8:])

        w_acc[...] = lax.fori_loop(0, w_rows // 16, add, w_acc[...])

    weight_part = w_acc[:, :LANES]
    for n in range(1, cols // LANES):
        weight_part += w_acc[:, n * LANES : (n + 1) * LANES]
    early[0:1] = jnp.sum(weight_part, axis=0, keepdims=True)
    loads[6].wait()
    loads[7].wait()
    old_rows = row_state[...]
    early[1:2] = jnp.sum(old_rows, axis=0, keepdims=True)
    for dr, dc in peers:
        n = dr * 4 + dc - 1
        remote(early, group_early.at[n], send_sem.at[1], sum_recv.at[0], group[(dr, (4 - dc) % 4)]).start()

    def turn(first, count, start, width):
        @pl.loop(0, width // LANES)
        def _(i):
            at = pl.multiple_of(start + i * LANES, LANES)
            block = xg[first * pair : (first + count) * pair, pl.ds(at, LANES)]
            xt[pl.ds(at, LANES), first * pair : (first + count) * pair] = block.T

    def multiply(place, halves, fresh=False):
        depth = slice(place * pair, (place + 1) * pair)

        for n in range(n_steps):
            at = slice(n * n_width, (n + 1) * n_width)
            for m in halves:
                here = slice(m * half, (m + 1) * half)
                part = jnp.dot(xt[here, depth], yg[depth, at], preferred_element_type=F32)
                if not fresh:
                    part += grad[here, at]
                grad[here, at] = part

    await_bytes(yg.at[pl.ds(0, 2 * tokens)], yz_recv.at[0])
    cross_y[3].start()
    cross_y[1].start()
    cross_x.wait_recv()
    for part in range(2):
        for direction in range(2):
            x_copy(1, direction, part).start()
    turn(0, 1, 0, rows)
    cross_y[0].wait_recv()
    multiply(0, (0, 1), fresh=True)
    y_copies[2].wait_recv()
    for copy in cross_last:
        copy.start()

    await_bytes(xg.at[pl.ds(0, 2 * tokens)], xz_recv.at[0])
    for step in range(SUBS):
        for s in range(2):
            for direction in range(2):
                forward(s, direction, step).start()
    turn(2, 1, 0, half)
    turn(1, 1, half, half)
    cross_y[3].wait_recv()
    multiply(2, (0,))
    cross_y[1].wait_recv()
    multiply(1, (1,))
    await_bytes(xg.at[pl.ds(0, 2 * tokens)], xz_recv.at[1])
    turn(2, 1, half, half)
    turn(1, 1, 0, half)
    multiply(2, (1,))
    multiply(1, (0,))
    col_part[...] = jnp.zeros_like(col_part)
    last = slice(PLACE[2] * pair, (PLACE[2] + 1) * pair)
    lanes = [slice(n * LANES, (n + 1) * LANES) for n in range(cols // LANES)]

    def await_forward(*steps):
        await_bytes(x_send.at[:, pl.ds(0, 4 * sub * len(steps))], fw_recv.at[FORWARD_SEM[steps[0]]])
        for step in steps:
            for direction in range(2):
                at = direction * half + step * sub
                to = (2 * step + direction) * sub
                xt_last[to : to + sub, :] = xg[last, at : at + sub].T

    def finish(first, end, steps):
        for n in range(*steps):
            at = slice(n * n_width, (n + 1) * n_width)
            total = col_part[:, at]
            for step in range(first, end):
                for direction in range(2):
                    here = slice(direction * half + step * sub, direction * half + (step + 1) * sub)
                    begin = (2 * (step - first) + direction) * sub
                    place = first * 2 * sub + begin
                    block = grad[here, at] + jnp.dot(
                        xt_last[place : place + sub], yg[last, at], preferred_element_type=F32
                    )
                    grad[here, at] = block
                    block = block * block
                    total += jnp.sum(block.reshape(sub // 8, 8, n_width), axis=0)
                    block = block[:, :LANES] + block[:, LANES:]
                    row_part[here] = block if n == 0 else row_part[here] + block
            col_part[:, at] = total

    def turn_sums(first, end):
        for direction in range(2):
            for step in range(first, end):
                begin = direction * half + step * sub
                turned = row_part[begin : begin + sub].T
                row_vec[begin // LANES : begin // LANES + 1] = jnp.sum(turned, axis=0, keepdims=True)

    def square():
        @pl.loop(0, rows // 32)
        def _(i):
            here = pl.ds(pl.multiple_of(i * 32, 32), 32)
            block = grad[here, :]
            squares[here, :] = block * block

    await_forward(0, 1)
    cross_last[0].wait_recv()
    finish(0, 2, LAST_STEPS[0])
    await_forward(2, 3)
    finish(2, 4, LAST_STEPS[0])
    cross_last[1].wait_recv()
    finish(0, 4, LAST_STEPS[1])
    await_forward(4)
    finish(4, 5, (0, LAST_STEPS[1][1]))
    cross_last[2].wait_recv()
    finish(0, 5, LAST_STEPS[2])
    await_forward(5)
    finish(5, 6, (0, n_steps))
    await_forward(6)
    finish(6, 7, (0, n_steps))
    turn_sums(0, 6)
    await_forward(7)
    finish(7, 8, (0, n_steps))

    square_part = col_part[:, :LANES]
    for lane in lanes[1:]:
        square_part += col_part[:, lane]
    square_part = jnp.sum(square_part, axis=0, keepdims=True)
    sent[0] = square_part
    for n, key in enumerate(everyone):
        remote(sent.at[0], gathered.at[n], send_sem.at[2], sum_recv.at[3], everyone[back(key)]).start()
    turn_sums(6, 8)
    for dc in (1, 2, 3):
        remote(row_vec, ring_rows.at[dc - 1], send_sem.at[4], sum_recv.at[1], group[(0, (4 - dc) % 4)]).start()
    col_vec[...] = jnp.sum(col_part[...], axis=0, keepdims=True)
    pair_copy = remote(col_vec, pair_cols, send_sem.at[3], sum_recv.at[2], partner)
    pair_copy.start()
    square()
    model_width, hidden_width = 2 * rows, 4 * cols
    entries = model_width * hidden_width
    matrices = (1 + len(everyone)) // (1 + len(peers))
    await_bytes(group_early, sum_recv.at[0])
    early_parts = {(0, 0): early[...]}
    for dr, dc in peers:
        early_parts[(dr, dc)] = group_early[dr * 4 + dc - 1]
    weight_total = full_sum(group_sum(early_parts)[0:1])
    old_total = full_sum((early_parts[(0, 0)] + early_parts[(1, 0)])[1:2])
    await_bytes(ring_rows, sum_recv.at[1])
    pair_copy.wait_recv()
    row_total = ring_sum([row_vec[...], ring_rows[0], ring_rows[1], ring_rows[2]])
    col_total = col_vec[...] + pair_cols[...]
    base = DECAY * row_state[...] + (1.0 - DECAY) * EPS
    rate = (1.0 - DECAY) * (row_total / hidden_width)
    for n in range(rows // LANES):
        here = slice(n * LANES, (n + 1) * LANES)
        row_base[here] = jnp.broadcast_to(base[n : n + 1], (LANES, LANES)).T
        row_rate[here] = jnp.broadcast_to(rate[n : n + 1], (LANES, LANES)).T
    await_bytes(gathered.at[pl.ds(0, len(everyone))], sum_recv.at[3])
    parts = {(0, 0, 0, 0, 0): square_part}
    for n, key in enumerate(everyone):
        parts[key] = gathered[n]
    groups = {}
    for expert in itertools.product(range(2), range(4), range(2)):
        groups[expert] = group_sum({key[3:]: part for key, part in parts.items() if key[:3] == expert})
    chips = [[groups[(dy, dx, 0)] + groups[(dy, dx, 1)] for dx in range(4)] for dy in range(2)]
    squared_total = full_sum(ring_sum(chips[0]) + ring_sum(chips[1]))
    group_squares = full_sum(groups[(0, 0, 0)])
    clip = 1.0 / jnp.maximum(1.0, jnp.sqrt(squared_total / (matrices * entries)))
    clip_square = clip * clip
    one = clip_square[:, :1]
    fresh_cols = col_total * one + model_width * EPS
    cols_now = DECAY * col_state[...] + (1.0 - DECAY) * (fresh_cols / model_width)
    col_scale[...] = 1.0 / cols_now

    def weigh(i, total):
        here = pl.ds(pl.multiple_of(i * 64, 64), 64)
        line = None
        for lane in lanes:
            block = squares[here, lane] * col_scale[:, lane]
            line = block if line is None else line + block
        line = line / (row_base[here] + row_rate[here] * one)
        return total + jnp.sum(line.reshape(8, 8, LANES), axis=0)

    update_part = lax.fori_loop(0, rows // 64, weigh, jnp.zeros((8, LANES), F32), unroll=2)
    update_part = jnp.sum(update_part, axis=0, keepdims=True)
    sent[1] = update_part
    first = len(everyone)
    for dr, dc in peers:
        n = first + dr * 4 + dc - 1
        remote(sent.at[1], gathered.at[n], send_sem.at[2], sum_recv.at[5], group[(dr, (4 - dc) % 4)]).start()
    new_rows[...] = base + rate * one
    new_cols[...] = cols_now
    average = DECAY * (old_total / model_width) + (1.0 - DECAY) * (group_squares * clip_square / entries + EPS)

    @pl.loop(0, rows // 64)
    def _(i):
        here = pl.ds(pl.multiple_of(i * 64, 64), 64)
        row_scale[here] = 1.0 / jnp.sqrt(row_base[here] + row_rate[here] * one)

    col_root = jnp.sqrt(col_scale[...])
    scale = clip * jnp.sqrt(average) * jnp.sqrt(weight_total / entries)
    sent_bytes = (5 * tokens * rows + 2 * tokens * rows + 7 * tokens * cols) * 2
    await_bytes(squares.at[pl.ds(0, sent_bytes // (4 * cols))], send_sem.at[0])
    await_bytes(group_early, send_sem.at[1])
    await_bytes(ring_rows, send_sem.at[4])
    pair_copy.wait_send()
    await_bytes(gathered, send_sem.at[2])
    await_bytes(gathered.at[pl.ds(first, len(peers))], sum_recv.at[5])
    parts = {(0, 0): update_part}
    for dr, dc in peers:
        parts[(dr, dc)] = gathered[first + dr * 4 + dc - 1]
    update_total = full_sum(group_sum(parts)) * clip_square * average
    factor = scale / jnp.maximum(1.0, jnp.sqrt(update_total / entries))
    col_scale[...] = col_root * factor[:, :1]


def scale_kernel(grad, row_scale, col_scale, rows_in, cols_in, out, rows_out, cols_out, scaled, sem):
    rows, cols = grad.shape
    height = 64
    rows_copy = pltpu.make_async_copy(rows_in, rows_out, sem.at[1])
    cols_copy = pltpu.make_async_copy(cols_in, cols_out, sem.at[2])
    rows_copy.start()
    cols_copy.start()

    @pl.loop(0, rows // height)
    def _(step):
        for i in range(height // 8):
            here = pl.ds(pl.multiple_of(step * height + i * 8, 8), 8)
            scale = row_scale[here]
            for n in range(cols // LANES):
                lane = slice(n * LANES, (n + 1) * LANES)
                scaled[here, lane] = grad[here, lane] * scale * col_scale[:, lane]
        block = pl.ds(pl.multiple_of(step * height, height), height)
        pltpu.make_async_copy(scaled.at[block], out.at[block], sem.at[0]).start()

    rows_copy.wait()
    cols_copy.wait()
    pltpu.make_async_copy(scaled, out, sem.at[0]).wait()


def body(weights, inputs, cotangents, row_state, col_state):
    _, rows, cols = weights.shape
    tokens = inputs.shape[1]
    lines = rows // LANES
    vmem = pl.BlockSpec(memory_space=pltpu.VMEM)
    anywhere = pl.BlockSpec(memory_space=pl.ANY)
    shapes = [
        pltpu.VMEM((rows, cols), F32),
        pltpu.VMEM((rows, LANES), F32),
        pltpu.VMEM((1, cols), F32),
        pltpu.VMEM((lines, LANES), F32),
        pltpu.VMEM((1, cols), F32),
    ]
    sub = rows // 2 // SUBS
    dma = pltpu.SemaphoreType.DMA
    grad, row_scale, col_scale, new_rows, new_cols = pl.pallas_call(
        gather_kernel,
        name="gather_gradient",
        out_shape=shapes,
        in_specs=[anywhere] * 5,
        out_specs=[vmem] * 5,
        scratch_shapes=[
            pltpu.VMEM((8 * tokens, rows), BF16),
            pltpu.VMEM((8 * tokens, cols), BF16),
            pltpu.VMEM((rows, 6 * tokens), BF16),
            pltpu.VMEM((rows, 2 * tokens), BF16),
            pltpu.VMEM((tokens, rows), BF16),
            pltpu.VMEM((3, tokens, cols), BF16),
            pltpu.VMEM((2, 256, cols), BF16),
            pltpu.VMEM((lines, LANES), F32),
            pltpu.VMEM((1, cols), F32),
            pltpu.VMEM((8, cols), F32),
            pltpu.VMEM((rows, cols), F32),
            pltpu.VMEM((rows, LANES), F32),
            pltpu.VMEM((rows, LANES), F32),
            pltpu.VMEM((rows, LANES), F32),
            pltpu.VMEM((8, cols), F32),
            pltpu.VMEM((lines, LANES), F32),
            pltpu.VMEM((1, cols), F32),
            pltpu.VMEM((2, LANES), F32),
            pltpu.VMEM((2, 1, LANES), F32),
            pltpu.VMEM((3, lines, LANES), F32),
            pltpu.VMEM((1, cols), F32),
            pltpu.VMEM((7, 2, LANES), F32),
            pltpu.VMEM((134, 1, LANES), F32),
            dma((8,)), dma((2,)), dma((5,)), dma((2,)), dma((2,)), dma((6,)), dma((7,)), dma((6,)),
        ],
        compiler_params=pltpu.CompilerParams(collective_id=0, has_side_effects=True, vmem_limit_bytes=40 * 2**20),
        cost_estimate=pl.CostEstimate(flops=16 * tokens * rows * cols, bytes_accessed=2**23, transcendentals=0),
    )(weights, inputs, cotangents, row_state.reshape(lines, LANES), col_state)
    out, rows_out, cols_out = pl.pallas_call(
        scale_kernel,
        name="scale_update",
        out_shape=[
            jax.ShapeDtypeStruct((rows, cols), F32),
            jax.ShapeDtypeStruct((lines, LANES), F32),
            jax.ShapeDtypeStruct((1, cols), F32),
        ],
        in_specs=[vmem] * 5,
        out_specs=[anywhere] * 3,
        scratch_shapes=[pltpu.VMEM((rows, cols), F32), dma((3,))],
        compiler_params=pltpu.CompilerParams(vmem_limit_bytes=20 * 2**20),
    )(grad, row_scale, col_scale, new_rows, new_cols)
    return out.reshape(1, rows, cols), rows_out.reshape(1, rows), cols_out


def solution(mesh):
    split = Mesh(
        mesh.devices.reshape(2, 4, 2, mesh.shape["row"], mesh.shape["col"]),
        (*EXPERT, "row", "col"),
    )
    return jax.shard_map(
        body,
        mesh=split,
        in_specs=(
            P(EXPERT, "row", "col"),
            P(EXPERT, ("row", "col"), None),
            P(EXPERT, ("row", "col"), None),
            P(EXPERT, "row"),
            P(EXPERT, "col"),
        ),
        out_specs=(P(EXPERT, "row", "col"), P(EXPERT, "row"), P(EXPERT, "col")),
        check_vma=False,
    )
```

```python
import itertools

import jax
import jax.numpy as jnp
from jax import lax
from jax.experimental import pallas as pl
from jax.experimental.pallas import tpu as pltpu
from jax.sharding import Mesh
from jax.sharding import PartitionSpec as P

STEP = 10
EPS = 1e-30
DECAY = 1.0 - STEP ** (-0.8)
EXPERT = ("ylo", "x", "core")
MESH = pl.DeviceIdType.MESH
F32 = jnp.float32
BF16 = jnp.bfloat16
SUBS = 8
LANES = 128
LOCAL_SEM = (0, 0, 1, 2, 3, 1)
FORWARD_SEM = (0, 0, 1, 1, 2, 3, 4, 5)
LAST_STEPS = ((0, 3), (3, 6), (6, 7))
PLACE = (0, 1, 3, 2)


def neighbours():
    lengths = (2, 4, 2, 2, 4)
    axes = (*EXPERT, "row", "col")
    here = [lax.axis_index(axis) for axis in axes]
    places = [[lax.rem(at + step, length) for step in range(length)] for at, length in zip(here, lengths)]
    steps = [s for s in itertools.product(*map(range, lengths)) if any(s)]
    hops = (1, (0, 1, 2, 1), 0, 2, (0, 1, 2, 1))
    far = lambda s: sum(h[k] if isinstance(h, tuple) else h * k for h, k in zip(hops, s))
    steps.sort(key=far, reverse=True)
    return {s: {axis: places[n][s[n]] for n, axis in enumerate(axes) if s[n]} for s in steps}


def back(step):
    return tuple((length - k) % length for k, length in zip(step, (2, 4, 2, 2, 4)))


def ring_sum(parts):
    return (parts[0] + parts[2]) + (parts[1] + parts[3])


def group_sum(parts):
    return ring_sum([parts[(0, c)] for c in range(4)]) + ring_sum([parts[(1, c)] for c in range(4)])


def full_sum(vector):
    return jnp.broadcast_to(jnp.sum(vector, keepdims=True), vector.shape)


def gather_kernel(
    weights, inputs, cotangents, row_state_in, col_state_in,
    grad, row_scale, col_scale, new_rows, new_cols,
    xg, yg, xt, xt_last, x_send, y_send, w_buf, row_state, col_state,
    w_acc, squares, row_base, row_rate, row_part, col_part, row_vec, col_vec, early, sent,
    ring_rows, pair_cols, group_early, gathered,
    local_sem, w_sem, send_sem, yz_recv, xz_recv, fw_recv, cross_recv, sum_recv,
):
    tokens = inputs.shape[1]
    rows, cols = grad.shape
    half, pair = rows // 2, 2 * tokens
    sub = half // SUBS
    row, col = lax.axis_index("row"), lax.axis_index("col")
    everyone = neighbours()
    group = {key[3:]: device for key, device in everyone.items() if not any(key[:3])}
    peers = list(group)
    near = {(0, 1), (0, 2), (0, 3), (1, 0)}
    greeted = [device for key, device in everyone.items() if not any(key[3:]) or not any(key[:3]) and key[3:] in near]
    up, down, across = group[(0, 1)], group[(0, 3)], group[(0, 2)]
    partner = group[(1, 0)]

    def remote(src, dst, send, recv, device):
        return pltpu.make_async_remote_copy(
            src_ref=src, dst_ref=dst, send_sem=send, recv_sem=recv, device_id=device, device_id_type=MESH
        )

    def tokens_of(buffer, j, s, width=None):
        start = PLACE[j] * pair + s * tokens
        if width is None:
            return buffer.at[pl.ds(start, tokens)]
        return buffer.at[pl.ds(start, tokens), width]

    def row_cols(r):
        return pl.ds(pl.multiple_of(r * rows, rows), rows)

    def col_cols(c):
        return pl.ds(pl.multiple_of(c * cols, cols), cols)

    y_dest = (1, 3, 2)
    local = []
    for n, dc in enumerate(y_dest):
        local.append((cotangents.at[0, :, col_cols(lax.rem(col + dc, 4))], y_send.at[n]))
    local.append((inputs.at[0, :, row_cols(1 - row)], x_send))
    local.append((inputs.at[0, :, row_cols(row)], tokens_of(xg, 0, 0)))
    local.append((cotangents.at[0, :, col_cols(col)], tokens_of(yg, 0, 0)))
    loads = [pltpu.make_async_copy(s, d, local_sem.at[LOCAL_SEM[n]]) for n, (s, d) in enumerate(local)]
    loads.append(pltpu.make_async_copy(row_state_in, row_state, local_sem.at[4]))
    loads.append(pltpu.make_async_copy(col_state_in, col_state, local_sem.at[5]))
    for n in (0, 1, 3, 4, 5, 2, 6, 7):
        loads[n].start()
    w_rows = w_buf.shape[1]
    w_steps = rows // w_rows

    def w_load(step, slot):
        start = pl.multiple_of(step * w_rows, w_rows)
        return pltpu.make_async_copy(weights.at[0, pl.ds(start, w_rows)], w_buf.at[slot], w_sem.at[slot])

    w_load(0, 0).start()

    barrier = pltpu.get_barrier_semaphore()
    for device in greeted:
        pl.semaphore_signal(barrier, inc=1, device_id=device, device_id_type=MESH)
    pl.semaphore_wait(barrier, len(greeted))

    y_copies = []
    for n, (dc, device) in enumerate(zip(y_dest, (up, down, across))):
        y_copies.append(
            remote(y_send.at[n], tokens_of(yg, (4 - dc) % 4, 0), send_sem.at[0], yz_recv.at[n // 2], device)
        )
    lower, upper = pl.ds(0, half), pl.ds(half, half)

    def x_copy(s, direction, part):
        device, j = ((up, 3), (down, 1))[direction]
        width = (lower, upper)[direction ^ part]
        recv = xz_recv.at[part]
        return remote(tokens_of(xg, 0, s, width), tokens_of(xg, j, s, width), send_sem.at[0], recv, device)

    def forward(s, direction, step):
        device, j = ((up, 3), (down, 1))[direction]
        width = pl.ds(direction * half + step * sub, sub)
        return remote(
            tokens_of(xg, j, s, width), tokens_of(xg, 2, s, width), send_sem.at[0], fw_recv.at[FORWARD_SEM[step]], device
        )

    def await_bytes(like, sem):
        pltpu.make_async_copy(like, like, sem).wait()

    cross_x = remote(x_send, tokens_of(xg, 0, 1), send_sem.at[0], cross_recv.at[2], partner)
    cross_y = {
        j: remote(tokens_of(yg, j, 0), tokens_of(yg, j, 1), send_sem.at[0], cross_recv.at[j], partner) for j in (0, 1, 3)
    }
    n_width = 2 * LANES
    n_steps = cols // n_width
    cross_last = []
    for n, (first, end) in enumerate(LAST_STEPS):
        width = pl.ds(first * n_width, (end - first) * n_width)
        recv = cross_recv.at[4 + n]
        cross_last.append(remote(tokens_of(yg, 2, 0, width), tokens_of(yg, 2, 1, width), send_sem.at[0], recv, partner))

    await_bytes(y_send.at[pl.ds(0, 2)], local_sem.at[0])
    y_copies[0].start()
    y_copies[1].start()
    loads[3].wait()
    cross_x.start()
    loads[4].wait()
    for part in range(2):
        for direction in range(2):
            x_copy(0, direction, part).start()
    await_bytes(y_send.at[pl.ds(0, 2)], local_sem.at[1])
    cross_y[0].start()
    y_copies[2].start()

    w_acc[...] = jnp.zeros_like(w_acc)

    @pl.loop(0, w_steps)
    def _(step):
        slot = lax.rem(step, 2)

        @pl.when(step + 1 < w_steps)
        def _():
            w_load(step + 1, 1 - slot).start()

        w_load(step, slot).wait()

        def add(i, total):
            block = w_buf[slot, pl.ds(pl.multiple_of(i * 16, 16), 16), :].astype(F32)
            block = block * block
            return total + (block[:8] + block[8:])

        w_acc[...] = lax.fori_loop(0, w_rows // 16, add, w_acc[...])

    weight_part = w_acc[:, :LANES]
    for n in range(1, cols // LANES):
        weight_part += w_acc[:, n * LANES : (n + 1) * LANES]
    early[0:1] = jnp.sum(weight_part, axis=0, keepdims=True)
    loads[6].wait()
    loads[7].wait()
    old_rows = row_state[...]
    early[1:2] = jnp.sum(old_rows, axis=0, keepdims=True)

    def turn(first, count, start, width):
        @pl.loop(0, width // LANES)
        def _(i):
            at = pl.multiple_of(start + i * LANES, LANES)
            block = xg[first * pair : (first + count) * pair, pl.ds(at, LANES)]
            xt[pl.ds(at, LANES), first * pair : (first + count) * pair] = block.T

    def multiply(place, halves, fresh=False):
        depth = slice(place * pair, (place + 1) * pair)

        for n in range(n_steps):
            at = slice(n * n_width, (n + 1) * n_width)
            for m in halves:
                here = slice(m * half, (m + 1) * half)
                part = jnp.dot(xt[here, depth], yg[depth, at], preferred_element_type=F32)
                if not fresh:
                    part += grad[here, at]
                grad[here, at] = part

    await_bytes(yg.at[pl.ds(0, 2 * tokens)], yz_recv.at[0])
    cross_y[3].start()
    cross_y[1].start()
    cross_x.wait_recv()
    for part in range(2):
        for direction in range(2):
            x_copy(1, direction, part).start()
    turn(0, 1, 0, rows)
    cross_y[0].wait_recv()
    multiply(0, (0, 1), fresh=True)
    y_copies[2].wait_recv()
    for copy in cross_last:
        copy.start()

    await_bytes(xg.at[pl.ds(0, 2 * tokens)], xz_recv.at[0])
    for step in range(SUBS):
        for s in range(2):
            for direction in range(2):
                forward(s, direction, step).start()
    turn(2, 1, 0, half)
    turn(1, 1, half, half)
    cross_y[3].wait_recv()
    multiply(2, (0,))
    cross_y[1].wait_recv()
    multiply(1, (1,))
    await_bytes(xg.at[pl.ds(0, 2 * tokens)], xz_recv.at[1])
    turn(2, 1, half, half)
    turn(1, 1, 0, half)
    multiply(2, (1,))
    multiply(1, (0,))
    col_part[...] = jnp.zeros_like(col_part)
    last = slice(PLACE[2] * pair, (PLACE[2] + 1) * pair)
    lanes = [slice(n * LANES, (n + 1) * LANES) for n in range(cols // LANES)]

    def await_forward(*steps):
        await_bytes(x_send.at[:, pl.ds(0, 4 * sub * len(steps))], fw_recv.at[FORWARD_SEM[steps[0]]])
        for step in steps:
            for direction in range(2):
                at = direction * half + step * sub
                to = (2 * step + direction) * sub
                xt_last[to : to + sub, :] = xg[last, at : at + sub].T

    def finish(first, end, steps):
        for n in range(*steps):
            at = slice(n * n_width, (n + 1) * n_width)
            total = col_part[:, at]
            for step in range(first, end):
                for direction in range(2):
                    here = slice(direction * half + step * sub, direction * half + (step + 1) * sub)
                    begin = (2 * (step - first) + direction) * sub
                    place = first * 2 * sub + begin
                    block = grad[here, at] + jnp.dot(
                        xt_last[place : place + sub], yg[last, at], preferred_element_type=F32
                    )
                    grad[here, at] = block
                    block = block * block
                    total += jnp.sum(block.reshape(sub // 8, 8, n_width), axis=0)
                    block = block[:, :LANES] + block[:, LANES:]
                    row_part[here] = block if n == 0 else row_part[here] + block
            col_part[:, at] = total

    def turn_sums(first, end):
        for direction in range(2):
            for step in range(first, end):
                begin = direction * half + step * sub
                turned = row_part[begin : begin + sub].T
                row_vec[begin // LANES : begin // LANES + 1] = jnp.sum(turned, axis=0, keepdims=True)

    def square():
        @pl.loop(0, rows // 32)
        def _(i):
            here = pl.ds(pl.multiple_of(i * 32, 32), 32)
            block = grad[here, :]
            squares[here, :] = block * block

    await_forward(0, 1)
    cross_last[0].wait_recv()
    finish(0, 2, LAST_STEPS[0])
    await_forward(2, 3)
    finish(2, 4, LAST_STEPS[0])
    cross_last[1].wait_recv()
    finish(0, 4, LAST_STEPS[1])
    await_forward(4)
    finish(4, 5, (0, LAST_STEPS[1][1]))
    cross_last[2].wait_recv()
    for dr, dc in peers:
        n = dr * 4 + dc - 1
        remote(early, group_early.at[n], send_sem.at[1], sum_recv.at[0], group[(dr, (4 - dc) % 4)]).start()
    finish(0, 5, LAST_STEPS[2])
    await_forward(5)
    finish(5, 6, (0, n_steps))
    await_forward(6)
    finish(6, 7, (0, n_steps))
    turn_sums(0, 6)
    await_forward(7)
    finish(7, 8, (0, n_steps))

    square_part = col_part[:, :LANES]
    for lane in lanes[1:]:
        square_part += col_part[:, lane]
    square_part = jnp.sum(square_part, axis=0, keepdims=True)
    sent[0] = square_part
    for n, key in enumerate(everyone):
        remote(sent.at[0], gathered.at[n], send_sem.at[2], sum_recv.at[3], everyone[back(key)]).start()
    turn_sums(6, 8)
    for dc in (1, 2, 3):
        remote(row_vec, ring_rows.at[dc - 1], send_sem.at[4], sum_recv.at[1], group[(0, (4 - dc) % 4)]).start()
    col_vec[...] = jnp.sum(col_part[...], axis=0, keepdims=True)
    pair_copy = remote(col_vec, pair_cols, send_sem.at[3], sum_recv.at[2], partner)
    pair_copy.start()
    square()
    model_width, hidden_width = 2 * rows, 4 * cols
    entries = model_width * hidden_width
    matrices = (1 + len(everyone)) // (1 + len(peers))
    await_bytes(group_early, sum_recv.at[0])
    early_parts = {(0, 0): early[...]}
    for dr, dc in peers:
        early_parts[(dr, dc)] = group_early[dr * 4 + dc - 1]
    weight_total = full_sum(group_sum(early_parts)[0:1])
    old_total = full_sum((early_parts[(0, 0)] + early_parts[(1, 0)])[1:2])
    await_bytes(ring_rows, sum_recv.at[1])
    pair_copy.wait_recv()
    row_total = ring_sum([row_vec[...], ring_rows[0], ring_rows[1], ring_rows[2]])
    col_total = col_vec[...] + pair_cols[...]
    base = DECAY * row_state[...] + (1.0 - DECAY) * EPS
    rate = (1.0 - DECAY) * (row_total / hidden_width)
    for n in range(rows // LANES):
        here = slice(n * LANES, (n + 1) * LANES)
        row_base[here] = jnp.broadcast_to(base[n : n + 1], (LANES, LANES)).T
        row_rate[here] = jnp.broadcast_to(rate[n : n + 1], (LANES, LANES)).T
    await_bytes(gathered.at[pl.ds(0, len(everyone))], sum_recv.at[3])
    parts = {(0, 0, 0, 0, 0): square_part}
    for n, key in enumerate(everyone):
        parts[key] = gathered[n]
    groups = {}
    for expert in itertools.product(range(2), range(4), range(2)):
        groups[expert] = group_sum({key[3:]: part for key, part in parts.items() if key[:3] == expert})
    chips = [[groups[(dy, dx, 0)] + groups[(dy, dx, 1)] for dx in range(4)] for dy in range(2)]
    squared_total = full_sum(ring_sum(chips[0]) + ring_sum(chips[1]))
    group_squares = full_sum(groups[(0, 0, 0)])
    clip_square = 1.0 / jnp.maximum(1.0, squared_total / (matrices * entries))
    one = clip_square[:, :1]
    fresh_cols = col_total * one + model_width * EPS
    cols_now = DECAY * col_state[...] + (1.0 - DECAY) * (fresh_cols / model_width)
    col_scale[...] = 1.0 / cols_now

    def weigh(i, total):
        here = pl.ds(pl.multiple_of(i * 64, 64), 64)
        line = None
        for lane in lanes:
            block = squares[here, lane] * col_scale[:, lane]
            line = block if line is None else line + block
        line = line / (row_base[here] + row_rate[here] * one)
        return total + jnp.sum(line.reshape(8, 8, LANES), axis=0)

    update_part = lax.fori_loop(0, rows // 64, weigh, jnp.zeros((8, LANES), F32), unroll=2)
    update_part = jnp.sum(update_part, axis=0, keepdims=True)
    sent[1] = update_part
    first = len(everyone)
    for dr, dc in peers:
        n = first + dr * 4 + dc - 1
        remote(sent.at[1], gathered.at[n], send_sem.at[2], sum_recv.at[5], group[(dr, (4 - dc) % 4)]).start()
    new_rows[...] = base + rate * one
    new_cols[...] = cols_now
    average = DECAY * (old_total / model_width) + (1.0 - DECAY) * (group_squares * clip_square / entries + EPS)

    @pl.loop(0, rows // 64)
    def _(i):
        here = pl.ds(pl.multiple_of(i * 64, 64), 64)
        row_scale[here] = 1.0 / jnp.sqrt(row_base[here] + row_rate[here] * one)

    col_root = jnp.sqrt(col_scale[...])
    scale = jnp.sqrt(clip_square) * jnp.sqrt(average) * jnp.sqrt(weight_total / entries)
    sent_bytes = (5 * tokens * rows + 2 * tokens * rows + 7 * tokens * cols) * 2
    await_bytes(squares.at[pl.ds(0, sent_bytes // (4 * cols))], send_sem.at[0])
    await_bytes(group_early, send_sem.at[1])
    await_bytes(ring_rows, send_sem.at[4])
    pair_copy.wait_send()
    await_bytes(gathered, send_sem.at[2])
    await_bytes(gathered.at[pl.ds(first, len(peers))], sum_recv.at[5])
    parts = {(0, 0): update_part}
    for dr, dc in peers:
        parts[(dr, dc)] = gathered[first + dr * 4 + dc - 1]
    update_total = full_sum(group_sum(parts)) * clip_square * average
    factor = scale / jnp.maximum(1.0, jnp.sqrt(update_total / entries))
    col_scale[...] = col_root * factor[:, :1]


def scale_kernel(grad, row_scale, col_scale, rows_in, cols_in, out, rows_out, cols_out, scaled, sem):
    rows, cols = grad.shape
    height = 64
    rows_copy = pltpu.make_async_copy(rows_in, rows_out, sem.at[1])
    cols_copy = pltpu.make_async_copy(cols_in, cols_out, sem.at[2])
    rows_copy.start()
    cols_copy.start()

    @pl.loop(0, rows // height)
    def _(step):
        for i in range(height // 8):
            here = pl.ds(pl.multiple_of(step * height + i * 8, 8), 8)
            scale = row_scale[here]
            for n in range(cols // LANES):
                lane = slice(n * LANES, (n + 1) * LANES)
                scaled[here, lane] = grad[here, lane] * scale * col_scale[:, lane]
        block = pl.ds(pl.multiple_of(step * height, height), height)
        pltpu.make_async_copy(scaled.at[block], out.at[block], sem.at[0]).start()

    rows_copy.wait()
    cols_copy.wait()
    pltpu.make_async_copy(scaled, out, sem.at[0]).wait()


def body(weights, inputs, cotangents, row_state, col_state):
    _, rows, cols = weights.shape
    tokens = inputs.shape[1]
    lines = rows // LANES
    vmem = pl.BlockSpec(memory_space=pltpu.VMEM)
    anywhere = pl.BlockSpec(memory_space=pl.ANY)
    shapes = [
        pltpu.VMEM((rows, cols), F32),
        pltpu.VMEM((rows, LANES), F32),
        pltpu.VMEM((1, cols), F32),
        pltpu.VMEM((lines, LANES), F32),
        pltpu.VMEM((1, cols), F32),
    ]
    sub = rows // 2 // SUBS
    dma = pltpu.SemaphoreType.DMA
    grad, row_scale, col_scale, new_rows, new_cols = pl.pallas_call(
        gather_kernel,
        name="gather_gradient",
        out_shape=shapes,
        in_specs=[anywhere] * 5,
        out_specs=[vmem] * 5,
        scratch_shapes=[
            pltpu.VMEM((8 * tokens, rows), BF16),
            pltpu.VMEM((8 * tokens, cols), BF16),
            pltpu.VMEM((rows, 6 * tokens), BF16),
            pltpu.VMEM((rows, 2 * tokens), BF16),
            pltpu.VMEM((tokens, rows), BF16),
            pltpu.VMEM((3, tokens, cols), BF16),
            pltpu.VMEM((2, 256, cols), BF16),
            pltpu.VMEM((lines, LANES), F32),
            pltpu.VMEM((1, cols), F32),
            pltpu.VMEM((8, cols), F32),
            pltpu.VMEM((rows, cols), F32),
            pltpu.VMEM((rows, LANES), F32),
            pltpu.VMEM((rows, LANES), F32),
            pltpu.VMEM((rows, LANES), F32),
            pltpu.VMEM((8, cols), F32),
            pltpu.VMEM((lines, LANES), F32),
            pltpu.VMEM((1, cols), F32),
            pltpu.VMEM((2, LANES), F32),
            pltpu.VMEM((2, 1, LANES), F32),
            pltpu.VMEM((3, lines, LANES), F32),
            pltpu.VMEM((1, cols), F32),
            pltpu.VMEM((7, 2, LANES), F32),
            pltpu.VMEM((134, 1, LANES), F32),
            dma((6,)), dma((2,)), dma((5,)), dma((2,)), dma((2,)), dma((6,)), dma((7,)), dma((6,)),
        ],
        compiler_params=pltpu.CompilerParams(collective_id=0, has_side_effects=True, vmem_limit_bytes=40 * 2**20),
        cost_estimate=pl.CostEstimate(flops=16 * tokens * rows * cols, bytes_accessed=2**23, transcendentals=0),
    )(weights, inputs, cotangents, row_state.reshape(lines, LANES), col_state)
    out, rows_out, cols_out = pl.pallas_call(
        scale_kernel,
        name="scale_update",
        out_shape=[
            jax.ShapeDtypeStruct((rows, cols), F32),
            jax.ShapeDtypeStruct((lines, LANES), F32),
            jax.ShapeDtypeStruct((1, cols), F32),
        ],
        in_specs=[vmem] * 5,
        out_specs=[anywhere] * 3,
        scratch_shapes=[pltpu.VMEM((rows, cols), F32), dma((3,))],
        compiler_params=pltpu.CompilerParams(vmem_limit_bytes=20 * 2**20),
    )(grad, row_scale, col_scale, new_rows, new_cols)
    return out.reshape(1, rows, cols), rows_out.reshape(1, rows), cols_out


def solution(mesh):
    split = Mesh(
        mesh.devices.reshape(2, 4, 2, mesh.shape["row"], mesh.shape["col"]),
        (*EXPERT, "row", "col"),
    )
    return jax.shard_map(
        body,
        mesh=split,
        in_specs=(
            P(EXPERT, "row", "col"),
            P(EXPERT, ("row", "col"), None),
            P(EXPERT, ("row", "col"), None),
            P(EXPERT, "row"),
            P(EXPERT, "col"),
        ),
        out_specs=(P(EXPERT, "row", "col"), P(EXPERT, "row"), P(EXPERT, "col")),
        check_vma=False,
    )
```

```python
import itertools

import jax
import jax.numpy as jnp
from jax import lax
from jax.experimental import pallas as pl
from jax.experimental.pallas import tpu as pltpu
from jax.sharding import Mesh
from jax.sharding import PartitionSpec as P

STEP = 10
EPS = 1e-30
DECAY = 1.0 - STEP ** (-0.8)
EXPERT = ("ylo", "x", "core")
MESH = pl.DeviceIdType.MESH
F32 = jnp.float32
BF16 = jnp.bfloat16
SUBS = 8
LANES = 128
LOCAL_SEM = (0, 0, 1, 2, 3, 1)
FORWARD_SEM = (0, 0, 1, 1, 2, 3, 4, 5)
LAST_STEPS = ((0, 3), (3, 6), (6, 7))
PLACE = (0, 1, 3, 2)


def neighbours():
    lengths = (2, 4, 2, 2, 4)
    axes = (*EXPERT, "row", "col")
    here = [lax.axis_index(axis) for axis in axes]
    places = [[lax.rem(at + step, length) for step in range(length)] for at, length in zip(here, lengths)]
    steps = [s for s in itertools.product(*map(range, lengths)) if any(s)]
    hops = (1, (0, 1, 2, 1), 0, 2, (0, 1, 2, 1))
    far = lambda s: sum(h[k] if isinstance(h, tuple) else h * k for h, k in zip(hops, s))
    steps.sort(key=far, reverse=True)
    return {s: {axis: places[n][s[n]] for n, axis in enumerate(axes) if s[n]} for s in steps}


def back(step):
    return tuple((length - k) % length for k, length in zip(step, (2, 4, 2, 2, 4)))


def ring_sum(parts):
    return (parts[0] + parts[2]) + (parts[1] + parts[3])


def group_sum(parts):
    return ring_sum([parts[(0, c)] for c in range(4)]) + ring_sum([parts[(1, c)] for c in range(4)])


def full_sum(vector):
    return jnp.broadcast_to(jnp.sum(vector, keepdims=True), vector.shape)


def gather_kernel(
    weights, inputs, cotangents, row_state_in, col_state_in,
    grad, row_scale, col_scale, new_rows, new_cols,
    xg, yg, xt, xt_last, x_send, y_send, w_buf, row_state, col_state,
    w_acc, squares, row_base, row_rate, row_part, col_part, row_vec, col_vec, early, sent,
    ring_rows, pair_cols, group_early, gathered,
    local_sem, w_sem, send_sem, yz_recv, xz_recv, fw_recv, cross_recv, sum_recv,
):
    tokens = inputs.shape[1]
    rows, cols = grad.shape
    half, pair = rows // 2, 2 * tokens
    sub = half // SUBS
    row, col = lax.axis_index("row"), lax.axis_index("col")
    everyone = neighbours()
    group = {key[3:]: device for key, device in everyone.items() if not any(key[:3])}
    peers = list(group)
    near = {(0, 1), (0, 2), (0, 3), (1, 0)}
    greeted = [device for key, device in everyone.items() if not any(key[3:]) or not any(key[:3]) and key[3:] in near]
    up, down, across = group[(0, 1)], group[(0, 3)], group[(0, 2)]
    partner = group[(1, 0)]

    def remote(src, dst, send, recv, device):
        return pltpu.make_async_remote_copy(
            src_ref=src, dst_ref=dst, send_sem=send, recv_sem=recv, device_id=device, device_id_type=MESH
        )

    def tokens_of(buffer, j, s, width=None):
        start = PLACE[j] * pair + s * tokens
        if width is None:
            return buffer.at[pl.ds(start, tokens)]
        return buffer.at[pl.ds(start, tokens), width]

    def row_cols(r):
        return pl.ds(pl.multiple_of(r * rows, rows), rows)

    def col_cols(c):
        return pl.ds(pl.multiple_of(c * cols, cols), cols)

    y_dest = (1, 3, 2)
    local = []
    for n, dc in enumerate(y_dest):
        local.append((cotangents.at[0, :, col_cols(lax.rem(col + dc, 4))], y_send.at[n]))
    local.append((inputs.at[0, :, row_cols(1 - row)], x_send))
    local.append((inputs.at[0, :, row_cols(row)], tokens_of(xg, 0, 0)))
    local.append((cotangents.at[0, :, col_cols(col)], tokens_of(yg, 0, 0)))
    loads = [pltpu.make_async_copy(s, d, local_sem.at[LOCAL_SEM[n]]) for n, (s, d) in enumerate(local)]
    loads.append(pltpu.make_async_copy(row_state_in, row_state, local_sem.at[4]))
    loads.append(pltpu.make_async_copy(col_state_in, col_state, local_sem.at[5]))
    for n in (0, 1, 3, 4, 5, 2, 6, 7):
        loads[n].start()
    w_rows = w_buf.shape[1]
    w_steps = rows // w_rows

    def w_load(step, slot):
        start = pl.multiple_of(step * w_rows, w_rows)
        return pltpu.make_async_copy(weights.at[0, pl.ds(start, w_rows)], w_buf.at[slot], w_sem.at[slot])

    w_load(0, 0).start()

    barrier = pltpu.get_barrier_semaphore()
    for device in greeted:
        pl.semaphore_signal(barrier, inc=1, device_id=device, device_id_type=MESH)
    pl.semaphore_wait(barrier, len(greeted))

    y_copies = []
    for n, (dc, device) in enumerate(zip(y_dest, (up, down, across))):
        y_copies.append(
            remote(y_send.at[n], tokens_of(yg, (4 - dc) % 4, 0), send_sem.at[0], yz_recv.at[n // 2], device)
        )
    lower, upper = pl.ds(0, half), pl.ds(half, half)

    def x_copy(s, direction, part):
        device, j = ((up, 3), (down, 1))[direction]
        width = (lower, upper)[direction ^ part]
        recv = xz_recv.at[part]
        return remote(tokens_of(xg, 0, s, width), tokens_of(xg, j, s, width), send_sem.at[0], recv, device)

    def forward(s, direction, step):
        device, j = ((up, 3), (down, 1))[direction]
        width = pl.ds(direction * half + step * sub, sub)
        return remote(
            tokens_of(xg, j, s, width), tokens_of(xg, 2, s, width), send_sem.at[0], fw_recv.at[FORWARD_SEM[step]], device
        )

    def await_bytes(like, sem):
        pltpu.make_async_copy(like, like, sem).wait()

    cross_x = remote(x_send, tokens_of(xg, 0, 1), send_sem.at[0], cross_recv.at[2], partner)
    cross_y = {
        j: remote(tokens_of(yg, j, 0), tokens_of(yg, j, 1), send_sem.at[0], cross_recv.at[j], partner) for j in (0, 1, 3)
    }
    n_width = 2 * LANES
    n_steps = cols // n_width
    cross_last = []
    for n, (first, end) in enumerate(LAST_STEPS):
        width = pl.ds(first * n_width, (end - first) * n_width)
        recv = cross_recv.at[4 + n]
        cross_last.append(remote(tokens_of(yg, 2, 0, width), tokens_of(yg, 2, 1, width), send_sem.at[0], recv, partner))

    await_bytes(y_send.at[pl.ds(0, 2)], local_sem.at[0])
    y_copies[0].start()
    y_copies[1].start()
    loads[3].wait()
    cross_x.start()
    loads[4].wait()
    for part in range(2):
        for direction in range(2):
            x_copy(0, direction, part).start()
    await_bytes(y_send.at[pl.ds(0, 2)], local_sem.at[1])
    cross_y[0].start()
    y_copies[2].start()

    w_acc[...] = jnp.zeros_like(w_acc)

    @pl.loop(0, w_steps)
    def _(step):
        slot = lax.rem(step, 2)

        @pl.when(step + 1 < w_steps)
        def _():
            w_load(step + 1, 1 - slot).start()

        w_load(step, slot).wait()

        def add(i, total):
            block = w_buf[slot, pl.ds(pl.multiple_of(i * 16, 16), 16), :].astype(F32)
            block = block * block
            return total + (block[:8] + block[8:])

        w_acc[...] = lax.fori_loop(0, w_rows // 16, add, w_acc[...])

    weight_part = w_acc[:, :LANES]
    for n in range(1, cols // LANES):
        weight_part += w_acc[:, n * LANES : (n + 1) * LANES]
    early[0:1] = jnp.sum(weight_part, axis=0, keepdims=True)
    loads[6].wait()
    loads[7].wait()
    old_rows = row_state[...]
    early[1:2] = jnp.sum(old_rows, axis=0, keepdims=True)

    def turn(first, count, start, width):
        @pl.loop(0, width // LANES)
        def _(i):
            at = pl.multiple_of(start + i * LANES, LANES)
            block = xg[first * pair : (first + count) * pair, pl.ds(at, LANES)]
            xt[pl.ds(at, LANES), first * pair : (first + count) * pair] = block.T

    def multiply(place, halves, fresh=False):
        depth = slice(place * pair, (place + 1) * pair)

        for n in range(n_steps):
            at = slice(n * n_width, (n + 1) * n_width)
            for m in halves:
                here = slice(m * half, (m + 1) * half)
                part = jnp.dot(xt[here, depth], yg[depth, at], preferred_element_type=F32)
                if not fresh:
                    part += grad[here, at]
                grad[here, at] = part

    await_bytes(yg.at[pl.ds(0, 2 * tokens)], yz_recv.at[0])
    cross_y[3].start()
    cross_y[1].start()
    cross_x.wait_recv()
    for part in range(2):
        for direction in range(2):
            x_copy(1, direction, part).start()
    turn(0, 1, 0, rows)
    cross_y[0].wait_recv()
    multiply(0, (0, 1), fresh=True)
    y_copies[2].wait_recv()
    for copy in cross_last:
        copy.start()

    await_bytes(xg.at[pl.ds(0, 2 * tokens)], xz_recv.at[0])
    for step in range(SUBS):
        for s in range(2):
            for direction in range(2):
                forward(s, direction, step).start()
    turn(2, 1, 0, half)
    turn(1, 1, half, half)
    cross_y[3].wait_recv()
    multiply(2, (0,))
    cross_y[1].wait_recv()
    multiply(1, (1,))
    await_bytes(xg.at[pl.ds(0, 2 * tokens)], xz_recv.at[1])
    turn(2, 1, half, half)
    turn(1, 1, 0, half)
    multiply(2, (1,))
    multiply(1, (0,))
    col_part[...] = jnp.zeros_like(col_part)
    last = slice(PLACE[2] * pair, (PLACE[2] + 1) * pair)
    lanes = [slice(n * LANES, (n + 1) * LANES) for n in range(cols // LANES)]

    def await_forward(*steps):
        await_bytes(x_send.at[:, pl.ds(0, 4 * sub * len(steps))], fw_recv.at[FORWARD_SEM[steps[0]]])
        for step in steps:
            for direction in range(2):
                at = direction * half + step * sub
                to = (2 * step + direction) * sub
                xt_last[to : to + sub, :] = xg[last, at : at + sub].T

    def finish(first, end, steps):
        for n in range(*steps):
            at = slice(n * n_width, (n + 1) * n_width)
            total = col_part[:, at]
            for step in range(first, end):
                for direction in range(2):
                    here = slice(direction * half + step * sub, direction * half + (step + 1) * sub)
                    begin = (2 * (step - first) + direction) * sub
                    place = first * 2 * sub + begin
                    block = grad[here, at] + jnp.dot(
                        xt_last[place : place + sub], yg[last, at], preferred_element_type=F32
                    )
                    grad[here, at] = block
                    block = block * block
                    total += jnp.sum(block.reshape(sub // 8, 8, n_width), axis=0)
                    block = block[:, :LANES] + block[:, LANES:]
                    row_part[here] = block if n == 0 else row_part[here] + block
            col_part[:, at] = total

    def turn_sums(first, end):
        for direction in range(2):
            for step in range(first, end):
                begin = direction * half + step * sub
                turned = row_part[begin : begin + sub].T
                row_vec[begin // LANES : begin // LANES + 1] = jnp.sum(turned, axis=0, keepdims=True)

    def square():
        @pl.loop(0, rows // 32)
        def _(i):
            here = pl.ds(pl.multiple_of(i * 32, 32), 32)
            block = grad[here, :]
            squares[here, :] = block * block

    await_forward(0, 1)
    cross_last[0].wait_recv()
    for dr, dc in peers:
        n = dr * 4 + dc - 1
        remote(early, group_early.at[n], send_sem.at[1], sum_recv.at[0], group[(dr, (4 - dc) % 4)]).start()
    finish(0, 2, LAST_STEPS[0])
    await_forward(2, 3)
    finish(2, 4, LAST_STEPS[0])
    cross_last[1].wait_recv()
    finish(0, 4, LAST_STEPS[1])
    await_forward(4)
    finish(4, 5, (0, LAST_STEPS[1][1]))
    cross_last[2].wait_recv()
    finish(0, 5, LAST_STEPS[2])
    await_forward(5)
    finish(5, 6, (0, n_steps))
    await_forward(6)
    finish(6, 7, (0, n_steps))
    await_forward(7)
    finish(7, 8, (0, n_steps))

    square_part = col_part[:, :LANES]
    for lane in lanes[1:]:
        square_part += col_part[:, lane]
    square_part = jnp.sum(square_part, axis=0, keepdims=True)
    sent[0] = square_part
    for n, key in enumerate(everyone):
        remote(sent.at[0], gathered.at[n], send_sem.at[2], sum_recv.at[3], everyone[back(key)]).start()
    turn_sums(0, 8)
    for dc in (1, 2, 3):
        remote(row_vec, ring_rows.at[dc - 1], send_sem.at[4], sum_recv.at[1], group[(0, (4 - dc) % 4)]).start()
    col_vec[...] = jnp.sum(col_part[...], axis=0, keepdims=True)
    pair_copy = remote(col_vec, pair_cols, send_sem.at[3], sum_recv.at[2], partner)
    pair_copy.start()
    square()
    model_width, hidden_width = 2 * rows, 4 * cols
    entries = model_width * hidden_width
    matrices = (1 + len(everyone)) // (1 + len(peers))
    await_bytes(group_early, sum_recv.at[0])
    early_parts = {(0, 0): early[...]}
    for dr, dc in peers:
        early_parts[(dr, dc)] = group_early[dr * 4 + dc - 1]
    weight_total = full_sum(group_sum(early_parts)[0:1])
    old_total = full_sum((early_parts[(0, 0)] + early_parts[(1, 0)])[1:2])
    await_bytes(ring_rows, sum_recv.at[1])
    pair_copy.wait_recv()
    row_total = ring_sum([row_vec[...], ring_rows[0], ring_rows[1], ring_rows[2]])
    col_total = col_vec[...] + pair_cols[...]
    base = DECAY * row_state[...] + (1.0 - DECAY) * EPS
    rate = (1.0 - DECAY) * (row_total / hidden_width)
    for n in range(rows // LANES):
        here = slice(n * LANES, (n + 1) * LANES)
        row_base[here] = jnp.broadcast_to(base[n : n + 1], (LANES, LANES)).T
        row_rate[here] = jnp.broadcast_to(rate[n : n + 1], (LANES, LANES)).T
    await_bytes(gathered.at[pl.ds(0, len(everyone))], sum_recv.at[3])
    parts = {(0, 0, 0, 0, 0): square_part}
    for n, key in enumerate(everyone):
        parts[key] = gathered[n]
    groups = {}
    for expert in itertools.product(range(2), range(4), range(2)):
        groups[expert] = group_sum({key[3:]: part for key, part in parts.items() if key[:3] == expert})
    chips = [[groups[(dy, dx, 0)] + groups[(dy, dx, 1)] for dx in range(4)] for dy in range(2)]
    squared_total = full_sum(ring_sum(chips[0]) + ring_sum(chips[1]))
    group_squares = full_sum(groups[(0, 0, 0)])
    clip_square = 1.0 / jnp.maximum(1.0, squared_total / (matrices * entries))
    one = clip_square[:, :1]
    fresh_cols = col_total * one + model_width * EPS
    cols_now = DECAY * col_state[...] + (1.0 - DECAY) * (fresh_cols / model_width)
    col_scale[...] = 1.0 / cols_now

    def weigh(i, total):
        here = pl.ds(pl.multiple_of(i * 64, 64), 64)
        line = None
        for lane in lanes:
            block = squares[here, lane] * col_scale[:, lane]
            line = block if line is None else line + block
        line = line / (row_base[here] + row_rate[here] * one)
        return total + jnp.sum(line.reshape(8, 8, LANES), axis=0)

    update_part = lax.fori_loop(0, rows // 64, weigh, jnp.zeros((8, LANES), F32), unroll=2)
    update_part = jnp.sum(update_part, axis=0, keepdims=True)
    sent[1] = update_part
    first = len(everyone)
    for dr, dc in peers:
        n = first + dr * 4 + dc - 1
        remote(sent.at[1], gathered.at[n], send_sem.at[2], sum_recv.at[5], group[(dr, (4 - dc) % 4)]).start()
    new_rows[...] = base + rate * one
    new_cols[...] = cols_now
    average = DECAY * (old_total / model_width) + (1.0 - DECAY) * (group_squares * clip_square / entries + EPS)

    @pl.loop(0, rows // 64)
    def _(i):
        here = pl.ds(pl.multiple_of(i * 64, 64), 64)
        row_scale[here] = 1.0 / jnp.sqrt(row_base[here] + row_rate[here] * one)

    col_root = jnp.sqrt(col_scale[...])
    scale = jnp.sqrt(clip_square) * jnp.sqrt(average) * jnp.sqrt(weight_total / entries)
    sent_bytes = (5 * tokens * rows + 2 * tokens * rows + 7 * tokens * cols) * 2
    await_bytes(squares.at[pl.ds(0, sent_bytes // (4 * cols))], send_sem.at[0])
    await_bytes(group_early, send_sem.at[1])
    await_bytes(ring_rows, send_sem.at[4])
    pair_copy.wait_send()
    await_bytes(gathered, send_sem.at[2])
    await_bytes(gathered.at[pl.ds(first, len(peers))], sum_recv.at[5])
    parts = {(0, 0): update_part}
    for dr, dc in peers:
        parts[(dr, dc)] = gathered[first + dr * 4 + dc - 1]
    update_total = full_sum(group_sum(parts)) * clip_square * average
    factor = scale / jnp.maximum(1.0, jnp.sqrt(update_total / entries))
    col_scale[...] = col_root * factor[:, :1]


def scale_kernel(grad, row_scale, col_scale, rows_in, cols_in, out, rows_out, cols_out, scaled, sem):
    rows, cols = grad.shape
    height = 64
    rows_copy = pltpu.make_async_copy(rows_in, rows_out, sem.at[1])
    cols_copy = pltpu.make_async_copy(cols_in, cols_out, sem.at[2])
    rows_copy.start()
    cols_copy.start()

    @pl.loop(0, rows // height)
    def _(step):
        for i in range(height // 8):
            here = pl.ds(pl.multiple_of(step * height + i * 8, 8), 8)
            scale = row_scale[here]
            for n in range(cols // LANES):
                lane = slice(n * LANES, (n + 1) * LANES)
                scaled[here, lane] = grad[here, lane] * scale * col_scale[:, lane]
        block = pl.ds(pl.multiple_of(step * height, height), height)
        pltpu.make_async_copy(scaled.at[block], out.at[block], sem.at[0]).start()

    rows_copy.wait()
    cols_copy.wait()
    pltpu.make_async_copy(scaled, out, sem.at[0]).wait()


def body(weights, inputs, cotangents, row_state, col_state):
    _, rows, cols = weights.shape
    tokens = inputs.shape[1]
    lines = rows // LANES
    vmem = pl.BlockSpec(memory_space=pltpu.VMEM)
    anywhere = pl.BlockSpec(memory_space=pl.ANY)
    shapes = [
        pltpu.VMEM((rows, cols), F32),
        pltpu.VMEM((rows, LANES), F32),
        pltpu.VMEM((1, cols), F32),
        pltpu.VMEM((lines, LANES), F32),
        pltpu.VMEM((1, cols), F32),
    ]
    sub = rows // 2 // SUBS
    dma = pltpu.SemaphoreType.DMA
    grad, row_scale, col_scale, new_rows, new_cols = pl.pallas_call(
        gather_kernel,
        name="gather_gradient",
        out_shape=shapes,
        in_specs=[anywhere] * 5,
        out_specs=[vmem] * 5,
        scratch_shapes=[
            pltpu.VMEM((8 * tokens, rows), BF16),
            pltpu.VMEM((8 * tokens, cols), BF16),
            pltpu.VMEM((rows, 6 * tokens), BF16),
            pltpu.VMEM((rows, 2 * tokens), BF16),
            pltpu.VMEM((tokens, rows), BF16),
            pltpu.VMEM((3, tokens, cols), BF16),
            pltpu.VMEM((2, 256, cols), BF16),
            pltpu.VMEM((lines, LANES), F32),
            pltpu.VMEM((1, cols), F32),
            pltpu.VMEM((8, cols), F32),
            pltpu.VMEM((rows, cols), F32),
            pltpu.VMEM((rows, LANES), F32),
            pltpu.VMEM((rows, LANES), F32),
            pltpu.VMEM((rows, LANES), F32),
            pltpu.VMEM((8, cols), F32),
            pltpu.VMEM((lines, LANES), F32),
            pltpu.VMEM((1, cols), F32),
            pltpu.VMEM((2, LANES), F32),
            pltpu.VMEM((2, 1, LANES), F32),
            pltpu.VMEM((3, lines, LANES), F32),
            pltpu.VMEM((1, cols), F32),
            pltpu.VMEM((7, 2, LANES), F32),
            pltpu.VMEM((134, 1, LANES), F32),
            dma((6,)), dma((2,)), dma((5,)), dma((2,)), dma((2,)), dma((6,)), dma((7,)), dma((6,)),
        ],
        compiler_params=pltpu.CompilerParams(collective_id=0, has_side_effects=True, vmem_limit_bytes=40 * 2**20),
        cost_estimate=pl.CostEstimate(flops=16 * tokens * rows * cols, bytes_accessed=2**23, transcendentals=0),
    )(weights, inputs, cotangents, row_state.reshape(lines, LANES), col_state)
    out, rows_out, cols_out = pl.pallas_call(
        scale_kernel,
        name="scale_update",
        out_shape=[
            jax.ShapeDtypeStruct((rows, cols), F32),
            jax.ShapeDtypeStruct((lines, LANES), F32),
            jax.ShapeDtypeStruct((1, cols), F32),
        ],
        in_specs=[vmem] * 5,
        out_specs=[anywhere] * 3,
        scratch_shapes=[pltpu.VMEM((rows, cols), F32), dma((3,))],
        compiler_params=pltpu.CompilerParams(vmem_limit_bytes=20 * 2**20),
    )(grad, row_scale, col_scale, new_rows, new_cols)
    return out.reshape(1, rows, cols), rows_out.reshape(1, rows), cols_out


def solution(mesh):
    split = Mesh(
        mesh.devices.reshape(2, 4, 2, mesh.shape["row"], mesh.shape["col"]),
        (*EXPERT, "row", "col"),
    )
    return jax.shard_map(
        body,
        mesh=split,
        in_specs=(
            P(EXPERT, "row", "col"),
            P(EXPERT, ("row", "col"), None),
            P(EXPERT, ("row", "col"), None),
            P(EXPERT, "row"),
            P(EXPERT, "col"),
        ),
        out_specs=(P(EXPERT, "row", "col"), P(EXPERT, "row"), P(EXPERT, "col")),
        check_vma=False,
    )
```
